32 devices in a mesh: dp: 2 (over x), tp: 16 (over z, y, core).
Axes of the slice: x: 2, y: 2, z: 4, core: 2. Of those that a mesh axis runs over, the one named last changes fastest.
Arguments:
- x_in: bfloat16 [1024, 7168], P('dp'), parts along dimension 0
- pos_ids: int32 [1024], P('dp'), parts along dimension 0
- ckv_cache: bfloat16 [2, 1024, 256, 512], P(None, 'dp'), parts along dimension 1
- kpe_cache: bfloat16 [2, 1024, 256, 64], P(None, 'dp'), parts along dimension 1
- attn_gain: bfloat16 [2, 7168], replicated
- w_dq: bfloat16 [2, 7168, 1536], replicated
- q_gain: bfloat16 [2, 1536], replicated
- w_dkv: bfloat16 [2, 7168, 576], replicated
- kv_gain: bfloat16 [2, 512], replicated
- w_uq: bfloat16 [2, 1536, 64, 192], P(None, None, 'tp')
- w_uk: bfloat16 [2, 512, 64, 128], P(None, None, 'tp')
- w_uv: bfloat16 [2, 512, 64, 128], P(None, None, 'tp')
- w_o: bfloat16 [2, 64, 128, 7168], P(None, 'tp')
- mlp_gain: bfloat16 [2, 7168], replicated
- w_gate: bfloat16 [2, 7168, 4608], P(None, None, 'tp')
- w_up: bfloat16 [2, 7168, 4608], P(None, None, 'tp')
- w_down: bfloat16 [2, 4608, 7168], P(None, 'tp')
Outputs:
- output 1: bfloat16 [1024, 7168], P('dp'), parts along dimension 0
- output 2: bfloat16 [2, 1024, 512], P(None, 'dp'), parts along dimension 1
- output 3: bfloat16 [2, 1024, 64], P(None, 'dp'), parts along dimension 1
There are 2 independent parts. The reference program is written for one: setup_inputs(seed, part) draws one part's arguments, and reference() takes and returns one part's arrays. A program takes and returns all parts, laid end to end along the dimension named above; an argument that names none is the same for every part.
All inputs are finite; a program needn't handle non-finite values.
Results may differ from the reference program's by a relative error of at most 0.02.
Values are sent between devices in bfloat16 or wider.
A program may use at most 1.75 GiB of HBM per device.

```python
import math
import jax
import jax.numpy as jnp
from jax import lax

SEQ_COUNT = 512
CACHE_LEN = 256
MODEL_DIM = 7168
FFN_DIM = 4608
NUM_HEADS = 64
Q_LORA = 1536
KV_LORA = 512
ROPE_DIM = 64
NOPE_DIM = 128
VALUE_DIM = 128
LAYER_COUNT = 2
ROPE_BASE = 10000

NORM_EPS = 1e-6
SCORE_SCALE = (NOPE_DIM + ROPE_DIM) ** -0.5


def rms_norm(values, norm_gain):
    values = values.astype(jnp.float32)
    inv_rms = lax.rsqrt(jnp.mean(values * values, axis=-1, keepdims=True) + NORM_EPS)
    return (values * inv_rms * norm_gain.astype(jnp.float32)).astype(jnp.bfloat16)


def rotary(values, positions):
    half_dim = ROPE_DIM // 2
    inv_freq = jnp.exp(jnp.arange(half_dim, dtype=jnp.float32) * (-2.0 * math.log(ROPE_BASE) / ROPE_DIM))
    angles = positions.astype(jnp.float32)[..., None] * inv_freq
    cos_part = jnp.cos(angles)
    sin_part = jnp.sin(angles)
    lo_half = values[..., :half_dim]
    hi_half = values[..., half_dim:]
    return jnp.concatenate([lo_half * cos_part - hi_half * sin_part, hi_half * cos_part + lo_half * sin_part], axis=-1)


def draw_normal(key, shape, std_dev):
    return (jax.random.normal(key, shape, jnp.float32) * std_dev).astype(jnp.bfloat16)


def draw_gain(key, width):
    return (1.0 + 0.25 * jax.random.normal(key, (LAYER_COUNT, width), jnp.float32)).astype(jnp.bfloat16)


def setup_inputs(seed: int = 0, part: int = 0) -> dict:
    shared_keys = jax.random.split(jax.random.key(seed), 16)
    local_keys = jax.random.split(jax.random.fold_in(jax.random.key(seed + 1), part), 6)
    qk_dim = NOPE_DIM + ROPE_DIM
    low_pos = CACHE_LEN // 2
    pos_ids = jax.random.randint(local_keys[1], (SEQ_COUNT,), low_pos, CACHE_LEN, jnp.int32)
    pos_ids = pos_ids.at[0].set(CACHE_LEN - 1).at[1].set(low_pos)
    seq_mean = jax.random.normal(local_keys[2], (LAYER_COUNT, SEQ_COUNT, 1, KV_LORA), jnp.float32)
    cache_noise = jax.random.normal(local_keys[3], (LAYER_COUNT, SEQ_COUNT, CACHE_LEN, KV_LORA), jnp.float32)
    return {
        'x_in': draw_normal(local_keys[0], (SEQ_COUNT, MODEL_DIM), 1.0),
        'pos_ids': pos_ids,
        'ckv_cache': (0.8 * seq_mean + 0.6 * cache_noise).astype(jnp.bfloat16),
        'kpe_cache': draw_normal(local_keys[4], (LAYER_COUNT, SEQ_COUNT, CACHE_LEN, ROPE_DIM), 1.0),
        'attn_gain': draw_gain(shared_keys[0], MODEL_DIM),
        'w_dq': draw_normal(shared_keys[1], (LAYER_COUNT, MODEL_DIM, Q_LORA), MODEL_DIM ** -0.5),
        'q_gain': draw_gain(shared_keys[2], Q_LORA),
        'w_dkv': draw_normal(shared_keys[3], (LAYER_COUNT, MODEL_DIM, KV_LORA + ROPE_DIM), MODEL_DIM ** -0.5),
        'kv_gain': draw_gain(shared_keys[4], KV_LORA),
        'w_uq': draw_normal(shared_keys[5], (LAYER_COUNT, Q_LORA, NUM_HEADS, qk_dim), Q_LORA ** -0.5),
        'w_uk': draw_normal(shared_keys[6], (LAYER_COUNT, KV_LORA, NUM_HEADS, NOPE_DIM), 3.0 * NOPE_DIM ** -0.5),
        'w_uv': draw_normal(shared_keys[7], (LAYER_COUNT, KV_LORA, NUM_HEADS, VALUE_DIM), KV_LORA ** -0.5),
        'w_o': draw_normal(shared_keys[8], (LAYER_COUNT, NUM_HEADS, VALUE_DIM, MODEL_DIM), (NUM_HEADS * VALUE_DIM) ** -0.5),
        'mlp_gain': draw_gain(shared_keys[9], MODEL_DIM),
        'w_gate': draw_normal(shared_keys[10], (LAYER_COUNT, MODEL_DIM, FFN_DIM), MODEL_DIM ** -0.5),
        'w_up': draw_normal(shared_keys[11], (LAYER_COUNT, MODEL_DIM, FFN_DIM), MODEL_DIM ** -0.5),
        'w_down': draw_normal(shared_keys[12], (LAYER_COUNT, FFN_DIM, MODEL_DIM), FFN_DIM ** -0.5),
    }


def attend_one(seq_item):
    q_lat, q_rope, ckv_seq, kpe_seq, position = seq_item
    scores = jnp.dot(q_lat, ckv_seq.T, preferred_element_type=jnp.float32)
    scores = (scores + jnp.dot(q_rope, kpe_seq.T, preferred_element_type=jnp.float32)) * SCORE_SCALE
    visible = jnp.arange(CACHE_LEN)[None, :] <= position
    scores = jnp.where(visible, scores, -jnp.inf)
    attn_prob = jax.nn.softmax(scores, axis=-1).astype(jnp.bfloat16)
    return jnp.dot(attn_prob, ckv_seq, preferred_element_type=jnp.float32).astype(jnp.bfloat16)


def one_layer(hidden, pos_ids, layer_in):
    (ckv_old, kpe_old, attn_gain, w_dq, q_gain, w_dkv, kv_gain, w_uq, w_uk, w_uv, w_o, mlp_gain, w_gate, w_up, w_down) = layer_in
    normed = rms_norm(hidden, attn_gain)
    c_q = rms_norm(jnp.dot(normed, w_dq, preferred_element_type=jnp.float32), q_gain)
    q_full = jnp.einsum('bc,chd->bhd', c_q.astype(jnp.float32), w_uq.astype(jnp.float32))
    q_nope = q_full[..., :NOPE_DIM].astype(jnp.bfloat16)
    q_rope = rotary(q_full[..., NOPE_DIM:], pos_ids[:, None]).astype(jnp.bfloat16)
    q_lat = jnp.einsum('bhn,chn->bhc', q_nope.astype(jnp.float32), w_uk.astype(jnp.float32)).astype(jnp.bfloat16)
    kv_lat = jnp.dot(normed, w_dkv, preferred_element_type=jnp.float32)
    ckv_new = rms_norm(kv_lat[:, :KV_LORA], kv_gain)
    kpe_new = rotary(kv_lat[:, KV_LORA:], pos_ids).astype(jnp.bfloat16)
    at_pos = (jnp.arange(CACHE_LEN)[None, :] == pos_ids[:, None])[:, :, None]
    ckv_all = jnp.where(at_pos, ckv_new[:, None, :], ckv_old)
    kpe_all = jnp.where(at_pos, kpe_new[:, None, :], kpe_old)
    context = lax.map(attend_one, (q_lat, q_rope, ckv_all, kpe_all, pos_ids))
    head_out = jnp.einsum('bhc,chv->bhv', context.astype(jnp.float32), w_uv.astype(jnp.float32)).astype(jnp.bfloat16)
    attn_sum = jnp.einsum('bhv,hvd->bd', head_out.astype(jnp.float32), w_o.astype(jnp.float32))
    mid_state = (hidden.astype(jnp.float32) + attn_sum).astype(jnp.bfloat16)
    mlp_in = rms_norm(mid_state, mlp_gain)
    gate_pre = jnp.dot(mlp_in, w_gate, preferred_element_type=jnp.float32)
    up_pre = jnp.dot(mlp_in, w_up, preferred_element_type=jnp.float32)
    act_out = (jax.nn.silu(gate_pre) * up_pre).astype(jnp.bfloat16)
    mlp_sum = jnp.dot(act_out, w_down, preferred_element_type=jnp.float32)
    layer_out = (mid_state.astype(jnp.float32) + mlp_sum).astype(jnp.bfloat16)
    return layer_out, (ckv_new, kpe_new)


def reference(x_in, pos_ids, ckv_cache, kpe_cache, attn_gain, w_dq, q_gain, w_dkv, kv_gain, w_uq, w_uk, w_uv, w_o, mlp_gain, w_gate, w_up, w_down):
    def layer_step(hidden, layer_in):
        return one_layer(hidden, pos_ids, layer_in)
    stacked = (ckv_cache, kpe_cache, attn_gain, w_dq, q_gain, w_dkv, kv_gain, w_uq, w_uk, w_uv, w_o, mlp_gain, w_gate, w_up, w_down)
    x_out, (ckv_rows, kpe_rows) = lax.scan(layer_step, x_in, stacked)
    return x_out, ckv_rows, kpe_rows
```

```python
import functools
import math
import jax
import jax.numpy as jnp
from jax import lax
from jax.experimental import pallas as pl
from jax.experimental.pallas import tpu as pltpu
from jax.sharding import PartitionSpec as P

NORM_EPS = 1e-6
ROPE_BASE = 10000.0
MESH = pl.DeviceIdType.MESH
RING = 8
CHUNK = 32
PIECE = 16
HALF = 256


def rms_norm(values, norm_gain):
    values = values.astype(jnp.float32)
    inv_rms = lax.rsqrt(jnp.mean(values * values, axis=-1, keepdims=True) + NORM_EPS)
    return (values * inv_rms * norm_gain.astype(jnp.float32)).astype(jnp.bfloat16)


def rotary(values, positions):
    half_dim = values.shape[-1] // 2
    inv_freq = jnp.exp(jnp.arange(half_dim, dtype=jnp.float32) * (-2.0 * math.log(ROPE_BASE) / values.shape[-1]))
    angles = positions.astype(jnp.float32)[..., None] * inv_freq
    cos_part = jnp.cos(angles)
    sin_part = jnp.sin(angles)
    lo_half = values[..., :half_dim]
    hi_half = values[..., half_dim:]
    return jnp.concatenate([lo_half * cos_part - hi_half * sin_part, hi_half * cos_part + lo_half * sin_part], axis=-1)


def ring_place():
    index = lax.axis_index('tp')
    core = index % 2
    chip = index // 2
    y = chip % 2
    z = chip // 2
    return core, z * (1 - y) + (7 - z) * y


def ring_device(position, core):
    y = position // 4
    z = position * (1 - y) + (7 - position) * y
    return (z * 2 + y) * 2 + core


def comm_kernel(reduce, norm, gather, canonical, subs, *refs):
    refs = list(refs)
    if reduce:
        part_ref = refs.pop(0)
        hidden_ref = refs.pop(0)
        gain_ref = refs.pop(0) if norm else None
        state_ref = refs.pop(0) if norm else None
        normed_ref = refs.pop(0) if norm and not gather else None
    else:
        shard_ref = refs.pop(0)
    full_ref = refs.pop(0) if gather else None
    if reduce:
        pair_buf, recv_buf, send_buf, pair_send, pair_recv, rs_send, rs_recv = refs[:7]
        refs = refs[7:]
    if gather:
        ag_send, ag_recv, fw_send, fw_recv = refs[:4]
    core, me = ring_place()
    dp_index = lax.axis_index('dp')
    right = (dp_index, ring_device((me + 1) % RING, core))
    left = (dp_index, ring_device((me + RING - 1) % RING, core))
    peer = (dp_index, ring_device(me, 1 - core))
    width = (part_ref if reduce else shard_ref).shape[-1]
    cols = width // subs

    barrier = pltpu.get_barrier_semaphore()
    for other in (left, right, peer):
        pl.semaphore_signal(barrier, inc=1, device_id=other, device_id_type=MESH)
    pl.semaphore_wait(barrier, 3)

    def remote(src, dst, send, recv, target):
        copy = pltpu.make_async_remote_copy(src_ref=src, dst_ref=dst, send_sem=send, recv_sem=recv, device_id=target, device_id_type=MESH)
        copy.start()
        return copy

    pending = []
    ways = ((right, -1), (left, 1))
    if reduce:
        pair_copies = {}
        for step in range(RING):
            for way, (target, sign) in enumerate(ways):
                piece = step * 2 + way
                chunk = (me + RING + sign * (1 + step)) % RING
                row = pl.multiple_of(chunk * CHUNK + way * PIECE, PIECE)
                pair_copies[piece] = remote(part_ref.at[pl.ds(HALF + row, PIECE)], pair_buf.at[piece], pair_send.at[piece], pair_recv.at[piece], peer)
        ring_copies = {}
        for step in range(RING):
            for way, (target, sign) in enumerate(ways):
                piece = step * 2 + way
                chunk = (me + RING + sign * (1 + step)) % RING
                row = pl.multiple_of(chunk * CHUNK + way * PIECE, PIECE)
                pair_copies[piece].wait()
                for sub in range(subs):
                    span = pl.ds(sub * cols, cols)
                    total = part_ref[pl.ds(row, PIECE), span].astype(jnp.float32) + pair_buf[piece, :, span].astype(jnp.float32)
                    if step > 0:
                        before = ring_copies[step - 1, way, sub]
                        before.wait_recv()
                        pending.append(before)
                        total = total + recv_buf[(step - 1) * 2 + way, :, span].astype(jnp.float32)
                    if step < RING - 1:
                        send_buf[piece, :, span] = total.astype(jnp.bfloat16)
                        ring_copies[step, way, sub] = remote(send_buf.at[piece, :, span], recv_buf.at[piece, :, span], rs_send.at[piece * subs + sub], rs_recv.at[piece * subs + sub], target)
                    else:
                        rows = pl.ds(way * PIECE, PIECE)
                        mixed = (hidden_ref[rows, span].astype(jnp.float32) + total).astype(jnp.bfloat16)
                        if norm:
                            state_ref[rows, span] = mixed
                        else:
                            own = pl.multiple_of((core * HALF if canonical else 0) + me * CHUNK + way * PIECE, PIECE)
                            full_ref[pl.ds(own, PIECE), span] = mixed
        if norm:
            for way in range(2):
                rows = pl.ds(way * PIECE, PIECE)
                values = state_ref[rows, :].astype(jnp.float32)
                inv_rms = lax.rsqrt(jnp.mean(values * values, axis=-1, keepdims=True) + NORM_EPS)
                normed = (values * inv_rms * gain_ref[...].astype(jnp.float32)).astype(jnp.bfloat16)
                if gather:
                    own = pl.multiple_of((core * HALF if canonical else 0) + me * CHUNK + way * PIECE, PIECE)
                    full_ref[pl.ds(own, PIECE), :] = normed
                else:
                    normed_ref[rows, :] = normed
    elif gather:
        own = pl.multiple_of((core * HALF if canonical else 0) + me * CHUNK, PIECE)
        full_ref[pl.ds(own, CHUNK), :] = shard_ref[...]
    if gather:
        base_here = core * HALF if canonical else 0
        base_peer = core * HALF if canonical else HALF

        def place(base, chunk, way):
            return pl.ds(pl.multiple_of(base + chunk * CHUNK + way * PIECE, PIECE), PIECE)

        ring_copies = {}
        fw_copies = []
        for step in range(RING):
            for way, (target, sign) in enumerate(ways):
                chunk = (me + RING + sign * step) % RING
                here = place(base_here, chunk, way)
                there = place(base_peer, chunk, way)
                for sub in range(subs):
                    span = pl.ds(sub * cols, cols)
                    slot = (step * 2 + way) * subs + sub
                    if step > 0:
                        before = ring_copies[step - 1, way, sub]
                        before.wait_recv()
                        pending.append(before)
                    if step < RING - 1:
                        ring_copies[step, way, sub] = remote(full_ref.at[here, span], full_ref.at[here, span], ag_send.at[slot], ag_recv.at[slot], target)
                    fw_copies.append(remote(full_ref.at[here, span], full_ref.at[there, span], fw_send.at[slot], fw_recv.at[slot], peer))
        for copy in fw_copies:
            copy.wait()
    for copy in pending:
        copy.wait_send()


def comm_call(call_id, reduce, norm, gather, canonical, subs, operands, width):
    vmem = pl.BlockSpec(memory_space=pltpu.VMEM)
    outs = []
    if reduce and norm:
        outs.append(jax.ShapeDtypeStruct((CHUNK, width), jnp.bfloat16))
        if not gather:
            outs.append(jax.ShapeDtypeStruct((CHUNK, width), jnp.bfloat16))
    if gather:
        outs.append(jax.ShapeDtypeStruct((2 * HALF, width), jnp.bfloat16))
    scratch = []
    dma = pltpu.SemaphoreType.DMA
    if reduce:
        scratch += [pltpu.VMEM((16, PIECE, width), jnp.bfloat16), pltpu.VMEM((14, PIECE, width), jnp.bfloat16), pltpu.VMEM((14, PIECE, width), jnp.bfloat16)]
        scratch += [dma((16,)), dma((16,)), dma((14 * subs,)), dma((14 * subs,))]
    if gather:
        scratch += [dma((14 * subs,)), dma((14 * subs,)), dma((16 * subs,)), dma((16 * subs,))]
    return pl.pallas_call(
        functools.partial(comm_kernel, reduce, norm, gather, canonical, subs),
        out_shape=outs,
        in_specs=[vmem] * len(operands),
        out_specs=[vmem] * len(outs),
        scratch_shapes=scratch,
        compiler_params=pltpu.CompilerParams(collective_id=call_id, has_side_effects=True, vmem_limit_bytes=48 * 1024 * 1024),
        name='comm%d' % call_id,
    )(*operands)


def swap_kernel(src_ref, dst_ref, send_sem, recv_sem):
    core, me = ring_place()
    peer = (lax.axis_index('dp'), ring_device(me, 1 - core))
    barrier = pltpu.get_barrier_semaphore()
    pl.semaphore_signal(barrier, inc=1, device_id=peer, device_id_type=MESH)
    pl.semaphore_wait(barrier, 1)
    copy = pltpu.make_async_remote_copy(src_ref=src_ref, dst_ref=dst_ref, send_sem=send_sem, recv_sem=recv_sem, device_id=peer, device_id_type=MESH)
    copy.start()
    copy.wait()


def swap_call(call_id, block):
    vmem = pl.BlockSpec(memory_space=pltpu.VMEM)
    return pl.pallas_call(
        swap_kernel,
        out_shape=jax.ShapeDtypeStruct(block.shape, block.dtype),
        in_specs=[vmem],
        out_specs=vmem,
        scratch_shapes=[pltpu.SemaphoreType.DMA, pltpu.SemaphoreType.DMA],
        compiler_params=pltpu.CompilerParams(collective_id=call_id, has_side_effects=True),
        name='swap%d' % call_id,
    )(block)


def attention_kernel(block, scale, meta_ref, q_ref, r_ref, ckv_ref, kpe_ref, cnew_ref, knew_ref, out_ref):
    start = meta_ref[0] + pl.program_id(0) * block
    heads, steps = q_ref.shape[1], ckv_ref.shape[2]
    key_steps = lax.broadcasted_iota(jnp.int32, (heads, steps), 1)
    scores = []
    for j in range(block):
        q = q_ref[j]
        r = r_ref[j]
        s = lax.dot_general(q, ckv_ref[0, j], (((1,), (1,)), ((), ())), preferred_element_type=jnp.float32)
        s = s + jnp.dot(r, kpe_ref[0, j], preferred_element_type=jnp.float32)
        scores.append(s)
    probs = []
    fresh_probs = []
    for j in range(block):
        pos = meta_ref[1 + start + j]
        fresh = jnp.sum(q_ref[j].astype(jnp.float32) * cnew_ref[j:j + 1, :].astype(jnp.float32), axis=-1, keepdims=True)
        fresh = fresh + jnp.sum(r_ref[j].astype(jnp.float32) * knew_ref[j:j + 1, :].astype(jnp.float32), axis=-1, keepdims=True)
        at_pos = key_steps == pos
        s = jnp.where(at_pos, fresh, scores[j]) * scale
        s = jnp.where(key_steps <= pos, s, -jnp.inf)
        e = jnp.exp(s - jnp.max(s, axis=-1, keepdims=True))
        p = (e / jnp.sum(e, axis=-1, keepdims=True)).astype(jnp.bfloat16).astype(jnp.float32)
        fresh_probs.append(jnp.sum(jnp.where(at_pos, p, 0.0), axis=-1, keepdims=True))
        probs.append(jnp.where(at_pos, 0.0, p).astype(jnp.bfloat16))
    for j in range(block):
        c = jnp.dot(probs[j], ckv_ref[0, j], preferred_element_type=jnp.float32)
        c = c + fresh_probs[j] * cnew_ref[j:j + 1, :].astype(jnp.float32)
        out_ref[j] = c.astype(jnp.bfloat16)


def attention_call(layer, core, positions, q_lat, q_rope, ckv_cache, kpe_cache, c_new, k_new, scale):
    block = 8
    rows, heads, latent = q_lat.shape
    rope = q_rope.shape[-1]
    steps = ckv_cache.shape[2]
    meta = jnp.concatenate([jnp.reshape(core * HALF, (1,)).astype(jnp.int32), positions])
    blocks = rows // block
    grid_spec = pltpu.PrefetchScalarGridSpec(
        num_scalar_prefetch=1,
        grid=(blocks,),
        in_specs=[
            pl.BlockSpec((block, heads, latent), lambda i, m: (i, 0, 0)),
            pl.BlockSpec((block, heads, rope), lambda i, m: (i, 0, 0)),
            pl.BlockSpec((1, block, steps, latent), lambda i, m: (layer, m[0] // block + i, 0, 0)),
            pl.BlockSpec((1, block, rope, steps), lambda i, m: (layer, m[0] // block + i, 0, 0)),
            pl.BlockSpec((block, latent), lambda i, m: (i, 0)),
            pl.BlockSpec((block, rope), lambda i, m: (i, 0)),
        ],
        out_specs=pl.BlockSpec((block, heads, latent), lambda i, m: (i, 0, 0)),
    )
    return pl.pallas_call(
        functools.partial(attention_kernel, block, scale),
        out_shape=jax.ShapeDtypeStruct((rows, heads, latent), jnp.bfloat16),
        grid_spec=grid_spec,
        compiler_params=pltpu.CompilerParams(vmem_limit_bytes=32 * 1024 * 1024),
        cost_estimate=pl.CostEstimate(flops=4 * rows * heads * steps * latent, bytes_accessed=rows * steps * (latent + rope) * 2, transcendentals=rows * heads * steps),
        name='attention',
    )(meta, q_lat, q_rope, ckv_cache, kpe_cache, c_new, k_new)


def solution(mesh):
    cache_spec = P(None, 'dp', None, None)
    head_spec = P(None, None, 'tp', None)
    weight_specs = (P(), P(), P(), P(), P(), head_spec, head_spec, head_spec, P(None, 'tp', None, None), P(), P(None, None, 'tp'), P(None, None, 'tp'), P(None, 'tp', None))
    in_specs = (P('dp', None), P('dp'), cache_spec, cache_spec) + weight_specs
    out_specs = (P('dp', None), P(None, 'dp', None), P(None, 'dp', None))
    pairs = [(i, i + 1 - 2 * (i % 2)) for i in range(16)]

    def device_body(x_in, pos_ids, ckv_cache, kpe_cache, attn_gain, w_dq, q_gain, w_dkv, kv_gain, w_uq, w_uk, w_uv, w_o, mlp_gain, w_gate, w_up, w_down):
        core, me = ring_place()
        layers, latent = ckv_cache.shape[0], ckv_cache.shape[-1]
        width = x_in.shape[-1]
        nope = w_uk.shape[-1]
        lora = w_dq.shape[-1]
        scale = w_uq.shape[-1] ** -0.5
        first = core * HALF + me * CHUNK
        kpe_t = jnp.swapaxes(kpe_cache, 2, 3)
        p_uq, p_uk, p_uv = [lax.ppermute(w, 'tp', pairs) for w in (w_uq, w_uk, w_uv)]
        state = lax.dynamic_slice_in_dim(x_in, first, CHUNK, 0)
        pos_rows = lax.dynamic_slice_in_dim(pos_ids, first, CHUNK, 0)
        pos_half = lax.dynamic_slice_in_dim(pos_ids, core * HALF, HALF, 0)
        normed = rms_norm(state, attn_gain[0])
        c_rows = []
        k_rows = []
        for layer in range(layers):
            c_q = rms_norm(jnp.dot(normed, w_dq[layer], preferred_element_type=jnp.float32), q_gain[layer])
            kv_lat = jnp.dot(normed, w_dkv[layer], preferred_element_type=jnp.float32)
            c_new = rms_norm(kv_lat[:, :latent], kv_gain[layer])
            k_new = rotary(kv_lat[:, latent:], pos_rows).astype(jnp.bfloat16)
            pad = jnp.zeros((CHUNK, 64), jnp.bfloat16)
            shard = jnp.concatenate([c_q, c_new, k_new, pad], axis=-1)
            latents, = comm_call(1, False, False, True, False, 1, (shard,), shard.shape[-1])
            c_all, k_all = latents[:, lora:lora + latent], latents[:, lora + latent:lora + latent + 64]
            ordered = jnp.where(core == 0, latents[:, lora:lora + latent + 64], jnp.roll(latents[:, lora:lora + latent + 64], HALF, axis=0))
            c_rows.append(ordered[:, :latent])
            k_rows.append(ordered[:, latent:])
            own_q = latents[:HALF, :lora]
            q_lats = []
            q_ropes = []
            for weight_q, weight_k in ((w_uq, w_uk), (p_uq, p_uk)):
                q_full = jnp.einsum('bc,chd->bhd', own_q, weight_q[layer], preferred_element_type=jnp.float32)
                q_nope = q_full[..., :nope].astype(jnp.bfloat16)
                q_ropes.append(rotary(q_full[..., nope:], pos_half[:, None]).astype(jnp.bfloat16))
                q_lats.append(jnp.einsum('bhn,chn->bhc', q_nope, weight_k[layer], preferred_element_type=jnp.float32).astype(jnp.bfloat16))
            q_lat = jnp.concatenate(q_lats, axis=1)
            q_rope = jnp.concatenate(q_ropes, axis=1)
            context = attention_call(layer, core, pos_ids, q_lat, q_rope, ckv_cache, kpe_t, c_all[:HALF], k_all[:HALF], scale)
            heads = w_uv.shape[2]
            own_o = jnp.einsum('bhc,chv->bhv', context[:, :heads], w_uv[layer], preferred_element_type=jnp.float32).astype(jnp.bfloat16)
            peer_o = jnp.einsum('bhc,chv->bhv', context[:, heads:], p_uv[layer], preferred_element_type=jnp.float32).astype(jnp.bfloat16)
            peer_o = swap_call(2, peer_o.reshape(HALF, -1))
            head_out = jnp.concatenate([own_o.reshape(HALF, -1), peer_o], axis=0)
            attn_part = jnp.dot(head_out, w_o[layer].reshape(-1, width), preferred_element_type=jnp.float32).astype(jnp.bfloat16)
            state, mlp_in = comm_call(3, True, True, True, False, 2, (attn_part, state, mlp_gain[layer][None]), width)
            gate_pre = jnp.dot(mlp_in, w_gate[layer], preferred_element_type=jnp.float32)
            up_pre = jnp.dot(mlp_in, w_up[layer], preferred_element_type=jnp.float32)
            act_out = (jax.nn.silu(gate_pre) * up_pre).astype(jnp.bfloat16)
            mlp_part = jnp.dot(act_out, w_down[layer], preferred_element_type=jnp.float32).astype(jnp.bfloat16)
            if layer + 1 < layers:
                state, normed = comm_call(4, True, True, False, False, 2, (mlp_part, state, attn_gain[layer + 1][None]), width)
            else:
                x_out, = comm_call(5, True, False, True, True, 2, (mlp_part, state), width)
        return x_out, jnp.stack(c_rows), jnp.stack(k_rows)

    return jax.shard_map(device_body, mesh=mesh, in_specs=in_specs, out_specs=out_specs, check_vma=False)
```

```python
import functools
import math
import jax
import jax.numpy as jnp
from jax import lax
from jax.experimental import pallas as pl
from jax.experimental.pallas import tpu as pltpu
from jax.sharding import PartitionSpec as P

NORM_EPS = 1e-6
ROPE_BASE = 10000.0
MESH = pl.DeviceIdType.MESH
RING = 8
CHUNK = 32
PIECE = 16
HALF = 256


def rms_norm(values, norm_gain):
    values = values.astype(jnp.float32)
    inv_rms = lax.rsqrt(jnp.mean(values * values, axis=-1, keepdims=True) + NORM_EPS)
    return (values * inv_rms * norm_gain.astype(jnp.float32)).astype(jnp.bfloat16)


def rotary(values, positions):
    half_dim = values.shape[-1] // 2
    inv_freq = jnp.exp(jnp.arange(half_dim, dtype=jnp.float32) * (-2.0 * math.log(ROPE_BASE) / values.shape[-1]))
    angles = positions.astype(jnp.float32)[..., None] * inv_freq
    cos_part = jnp.cos(angles)
    sin_part = jnp.sin(angles)
    lo_half = values[..., :half_dim]
    hi_half = values[..., half_dim:]
    return jnp.concatenate([lo_half * cos_part - hi_half * sin_part, hi_half * cos_part + lo_half * sin_part], axis=-1)


def ring_place():
    index = lax.axis_index('tp')
    core = index % 2
    chip = index // 2
    y = chip % 2
    z = chip // 2
    return core, z * (1 - y) + (7 - z) * y


def ring_device(position, core):
    y = position // 4
    z = position * (1 - y) + (7 - position) * y
    return (z * 2 + y) * 2 + core


def comm_kernel(reduce, norm, gather, canonical, subs, *refs):
    refs = list(refs)
    if reduce:
        part_ref = refs.pop(0)
        hidden_ref = refs.pop(0)
        gain_ref = refs.pop(0) if norm else None
        state_ref = refs.pop(0) if norm else None
        normed_ref = refs.pop(0) if norm and not gather else None
    else:
        shard_ref = refs.pop(0)
    full_ref = refs.pop(0) if gather else None
    if reduce:
        pair_buf, recv_buf, send_buf, pair_send, pair_recv, rs_send, rs_recv = refs[:7]
        refs = refs[7:]
    if gather:
        ag_send, ag_recv, fw_send, fw_recv = refs[:4]
    core, me = ring_place()
    dp_index = lax.axis_index('dp')
    right = (dp_index, ring_device((me + 1) % RING, core))
    left = (dp_index, ring_device((me + RING - 1) % RING, core))
    peer = (dp_index, ring_device(me, 1 - core))
    width = (part_ref if reduce else shard_ref).shape[-1]
    cols = width // subs

    barrier = pltpu.get_barrier_semaphore()
    for other in (left, right, peer):
        pl.semaphore_signal(barrier, inc=1, device_id=other, device_id_type=MESH)
    pl.semaphore_wait(barrier, 3)

    def remote(src, dst, send, recv, target):
        copy = pltpu.make_async_remote_copy(src_ref=src, dst_ref=dst, send_sem=send, recv_sem=recv, device_id=target, device_id_type=MESH)
        copy.start()
        return copy

    pending = []
    ways = ((right, -1), (left, 1))
    if reduce:
        pair_copies = {}
        for step in range(RING):
            for way, (target, sign) in enumerate(ways):
                piece = step * 2 + way
                chunk = (me + RING + sign * (1 + step)) % RING
                row = pl.multiple_of(chunk * CHUNK + way * PIECE, PIECE)
                pair_copies[piece] = remote(part_ref.at[pl.ds(HALF + row, PIECE)], pair_buf.at[piece], pair_send.at[piece], pair_recv.at[piece], peer)
        ring_copies = {}
        for step in range(RING):
            for way, (target, sign) in enumerate(ways):
                piece = step * 2 + way
                chunk = (me + RING + sign * (1 + step)) % RING
                row = pl.multiple_of(chunk * CHUNK + way * PIECE, PIECE)
                pair_copies[piece].wait()
                for sub in range(subs):
                    span = pl.ds(sub * cols, cols)
                    total = part_ref[pl.ds(row, PIECE), span].astype(jnp.float32) + pair_buf[piece, :, span].astype(jnp.float32)
                    if step > 0:
                        before = ring_copies[step - 1, way, sub]
                        before.wait_recv()
                        pending.append(before)
                        total = total + recv_buf[(step - 1) * 2 + way, :, span].astype(jnp.float32)
                    if step < RING - 1:
                        send_buf[piece, :, span] = total.astype(jnp.bfloat16)
                        ring_copies[step, way, sub] = remote(send_buf.at[piece, :, span], recv_buf.at[piece, :, span], rs_send.at[piece * subs + sub], rs_recv.at[piece * subs + sub], target)
                    else:
                        rows = pl.ds(way * PIECE, PIECE)
                        mixed = (hidden_ref[rows, span].astype(jnp.float32) + total).astype(jnp.bfloat16)
                        if norm:
                            state_ref[rows, span] = mixed
                        else:
                            own = pl.multiple_of((core * HALF if canonical else 0) + me * CHUNK + way * PIECE, PIECE)
                            full_ref[pl.ds(own, PIECE), span] = mixed
        if norm:
            for way in range(2):
                rows = pl.ds(way * PIECE, PIECE)
                values = state_ref[rows, :].astype(jnp.float32)
                inv_rms = lax.rsqrt(jnp.mean(values * values, axis=-1, keepdims=True) + NORM_EPS)
                normed = (values * inv_rms * gain_ref[...].astype(jnp.float32)).astype(jnp.bfloat16)
                if gather:
                    own = pl.multiple_of((core * HALF if canonical else 0) + me * CHUNK + way * PIECE, PIECE)
                    full_ref[pl.ds(own, PIECE), :] = normed
                else:
                    normed_ref[rows, :] = normed
    elif gather:
        own = pl.multiple_of((core * HALF if canonical else 0) + me * CHUNK, PIECE)
        full_ref[pl.ds(own, CHUNK), :] = shard_ref[...]
    if gather:
        base_here = core * HALF if canonical else 0
        base_peer = core * HALF if canonical else HALF

        def place(base, chunk, way):
            return pl.ds(pl.multiple_of(base + chunk * CHUNK + way * PIECE, PIECE), PIECE)

        ring_copies = {}
        fw_copies = []
        for step in range(RING):
            for way, (target, sign) in enumerate(ways):
                chunk = (me + RING + sign * step) % RING
                here = place(base_here, chunk, way)
                there = place(base_peer, chunk, way)
                for sub in range(subs):
                    span = pl.ds(sub * cols, cols)
                    slot = (step * 2 + way) * subs + sub
                    if step > 0:
                        before = ring_copies[step - 1, way, sub]
                        before.wait_recv()
                        pending.append(before)
                    if step < RING - 1:
                        ring_copies[step, way, sub] = remote(full_ref.at[here, span], full_ref.at[here, span], ag_send.at[slot], ag_recv.at[slot], target)
                    fw_copies.append(remote(full_ref.at[here, span], full_ref.at[there, span], fw_send.at[slot], fw_recv.at[slot], peer))
        for copy in fw_copies:
            copy.wait()
    for copy in pending:
        copy.wait_send()


def comm_call(call_id, reduce, norm, gather, canonical, subs, operands, width):
    vmem = pl.BlockSpec(memory_space=pltpu.VMEM)
    outs = []
    if reduce and norm:
        outs.append(jax.ShapeDtypeStruct((CHUNK, width), jnp.bfloat16))
        if not gather:
            outs.append(jax.ShapeDtypeStruct((CHUNK, width), jnp.bfloat16))
    if gather:
        outs.append(jax.ShapeDtypeStruct((2 * HALF, width), jnp.bfloat16))
    scratch = []
    dma = pltpu.SemaphoreType.DMA
    if reduce:
        scratch += [pltpu.VMEM((16, PIECE, width), jnp.bfloat16), pltpu.VMEM((14, PIECE, width), jnp.bfloat16), pltpu.VMEM((14, PIECE, width), jnp.bfloat16)]
        scratch += [dma((16,)), dma((16,)), dma((14 * subs,)), dma((14 * subs,))]
    if gather:
        scratch += [dma((14 * subs,)), dma((14 * subs,)), dma((16 * subs,)), dma((16 * subs,))]
    return pl.pallas_call(
        functools.partial(comm_kernel, reduce, norm, gather, canonical, subs),
        out_shape=outs,
        in_specs=[vmem] * len(operands),
        out_specs=[vmem] * len(outs),
        scratch_shapes=scratch,
        compiler_params=pltpu.CompilerParams(collective_id=call_id, has_side_effects=True, vmem_limit_bytes=48 * 1024 * 1024),
        name='comm%d' % call_id,
    )(*operands)


def layer_kernel(layer, last, subs, *refs):
    refs = list(refs)
    o_ref, hidden_ref, gain_ref = refs[:3]
    refs = refs[3:]
    next_ref = None if last else refs.pop(0)
    wo_hbm, gate_hbm, up_hbm, down_hbm = refs[:4]
    refs = refs[4:]
    if last:
        full_ref = refs.pop(0)
    else:
        state_out, normed_out = refs[:2]
        refs = refs[2:]
    (wo, gate, up, down, b_full, batch, act, state, own_part, pair_out, pair_buf, recv_buf, send_buf,
     w_sem, pair_send, pair_recv, rs_send, rs_recv, ag_send, ag_recv, fw_send, fw_recv) = refs
    width = hidden_ref.shape[-1]
    cols = width // subs
    block = 1024
    blocks = width // block
    ffn = gate.shape[0]
    core, me = ring_place()
    dp_index = lax.axis_index('dp')
    right = (dp_index, ring_device((me + 1) % RING, core))
    left = (dp_index, ring_device((me + RING - 1) % RING, core))
    peer = (dp_index, ring_device(me, 1 - core))
    ways = ((right, -1), (left, 1))

    def wo_copy(i):
        span = pl.ds(pl.multiple_of(i * block, block), block)
        return pltpu.make_async_copy(wo_hbm.at[layer, :, span], wo.at[:, span], w_sem.at[i])

    gate_copy = pltpu.make_async_copy(gate_hbm.at[layer], gate, w_sem.at[blocks])
    up_copy = pltpu.make_async_copy(up_hbm.at[layer], up, w_sem.at[blocks + 1])
    down_copy = pltpu.make_async_copy(down_hbm.at[layer], down.at[pl.ds(0, ffn)], w_sem.at[blocks + 2])
    for i in range(blocks):
        wo_copy(i).start()
    gate_copy.start()
    up_copy.start()
    down_copy.start()

    barrier = pltpu.get_barrier_semaphore()
    for other in (left, right, peer):
        pl.semaphore_signal(barrier, inc=1, device_id=other, device_id_type=MESH)
    pl.semaphore_wait(barrier, 3)

    def remote(src, dst, send, recv, target):
        return pltpu.make_async_remote_copy(src_ref=src, dst_ref=dst, send_sem=send, recv_sem=recv, device_id=target, device_id_type=MESH)

    def piece_row(step, way):
        chunk = (me + RING + (step if way else -step)) % RING
        return pl.multiple_of(chunk * CHUNK + way * PIECE, PIECE)

    def pair_copy(step):
        return remote(pair_out.at[step], pair_buf.at[step], pair_send.at[step], pair_recv.at[step], peer)

    def rs_copy(step, way, sub):
        slot = (step * 2 + way) * subs + sub
        where = (step, pl.ds(way * PIECE, PIECE), pl.ds(sub * cols, cols))
        return remote(send_buf.at[where], recv_buf.at[where], rs_send.at[slot], rs_recv.at[slot], ways[way][0])

    def reduce_scatter(source, weight, ready, finish):
        def one_step(step, carry):
            near, far = piece_row(step + 1, 0), piece_row(step + 1, 1)
            rows = [source[pl.ds(pl.multiple_of(base + at, PIECE), PIECE), :] for base in (0, HALF) for at in (near, far)]
            lhs = jnp.concatenate(rows, axis=0)

            def one_block(i, carry):
                span = pl.ds(pl.multiple_of(i * block, block), block)
                if ready is not None:
                    @pl.when(step == 0)
                    def _():
                        ready(i)
                prod = jnp.dot(lhs, weight[:, span], preferred_element_type=jnp.float32)
                own_part[:, span] = prod[:CHUNK]
                pair_out[step, :, span] = prod[CHUNK:].astype(jnp.bfloat16)
                return carry

            lax.fori_loop(0, blocks, one_block, 0)
            pair_copy(step).start()
            pair_copy(step).wait_recv()
            for sub in range(subs):
                span = pl.ds(sub * cols, cols)
                for way in range(2):
                    rows = pl.ds(way * PIECE, PIECE)

                    @pl.when(step > 0)
                    def _():
                        rs_copy(step - 1, way, sub).wait_recv()
                        own_part[rows, span] += recv_buf[step - 1, rows, span].astype(jnp.float32)

                    total = own_part[rows, span] + pair_buf[step, rows, span].astype(jnp.float32)

                    @pl.when(step < RING - 1)
                    def _():
                        send_buf[step, rows, span] = total.astype(jnp.bfloat16)
                        rs_copy(step, way, sub).start()

                    @pl.when(step == RING - 1)
                    def _():
                        finish(rows, span, total)
            return carry

        lax.fori_loop(0, RING, one_step, 0)

        def drain(step, carry):
            pair_copy(step).wait_send()

            @pl.when(step < RING - 1)
            def _():
                for way in range(2):
                    for sub in range(subs):
                        rs_copy(step, way, sub).wait_send()
            return carry

        lax.fori_loop(0, RING, drain, 0)

    def normalise(values, gain):
        values = values.astype(jnp.float32)
        inv_rms = lax.rsqrt(jnp.mean(values * values, axis=-1, keepdims=True) + NORM_EPS)
        return (values * inv_rms * gain[...].astype(jnp.float32)).astype(jnp.bfloat16)

    def all_gather(buf, base_here, base_there, consume):
        def ag_copy(step, way, sub):
            slot = (step * 2 + way) * subs + sub
            here = buf.at[pl.ds(pl.multiple_of(base_here + piece_row(step, way), PIECE), PIECE), pl.ds(sub * cols, cols)]
            return remote(here, here, ag_send.at[slot], ag_recv.at[slot], ways[way][0])

        def fw_copy(step, way, sub):
            slot = (step * 2 + way) * subs + sub
            here = buf.at[pl.ds(pl.multiple_of(base_here + piece_row(step, way), PIECE), PIECE), pl.ds(sub * cols, cols)]
            there = buf.at[pl.ds(pl.multiple_of(base_there + piece_row(step, way), PIECE), PIECE), pl.ds(sub * cols, cols)]
            return remote(here, there, fw_send.at[slot], fw_recv.at[slot], peer)

        def two_steps(pair, carry):
            for odd in range(2):
                step = pair * 2 + odd
                for sub in range(subs):
                    for way in range(2):
                        if odd:
                            ag_copy(step - 1, way, sub).wait_recv()
                        else:
                            @pl.when(pair > 0)
                            def _():
                                ag_copy(step - 1, way, sub).wait_recv()
                        if odd:
                            @pl.when(pair < RING // 2 - 1)
                            def _():
                                ag_copy(step, way, sub).start()
                        else:
                            ag_copy(step, way, sub).start()
                        fw_copy(step, way, sub).start()
            for odd in range(2):
                for way in range(2):
                    for sub in range(subs):
                        fw_copy(pair * 2 + odd, way, sub).wait_recv()
            if consume is not None:
                consume(pair)
            return carry

        lax.fori_loop(0, RING // 2, two_steps, 0)

        def drain(step, carry):
            for way in range(2):
                for sub in range(subs):
                    fw_copy(step, way, sub).wait_send()

                    @pl.when(step < RING - 1)
                    def _():
                        ag_copy(step, way, sub).wait_send()
            return carry

        lax.fori_loop(0, RING, drain, 0)

    def finish_mid(rows, span, total):
        state[rows, span] = (hidden_ref[rows, span].astype(jnp.float32) + total).astype(jnp.bfloat16)

    reduce_scatter(o_ref, wo, lambda i: wo_copy(i).wait(), finish_mid)
    b_full[pl.ds(pl.multiple_of(me * CHUNK, CHUNK), CHUNK), :] = normalise(state[...], gain_ref)
    down[pl.ds(ffn, down.shape[0] - ffn), :] = jnp.zeros((down.shape[0] - ffn, width), jnp.bfloat16)
    gate_copy.wait()
    up_copy.wait()
    down_copy.wait()

    def mlp_rows(pair):
        places = [(base, step, way) for base in (0, HALF) for step in range(2) for way in range(2)]
        for i, (base, odd, way) in enumerate(places):
            at = pl.multiple_of(base + piece_row(pair * 2 + odd, way), PIECE)
            batch[pl.ds(i * PIECE, PIECE), :] = b_full[pl.ds(at, PIECE), :]
        dims = (((1,), (1,)), ((), ()))
        gate_pre = lax.dot_general(gate[...], batch[...], dims, preferred_element_type=jnp.float32)
        up_pre = lax.dot_general(up[...], batch[...], dims, preferred_element_type=jnp.float32)
        hidden_act = jax.nn.silu(gate_pre) * up_pre
        padded = jnp.concatenate([hidden_act, jnp.zeros((act.shape[1] - ffn, 128), jnp.float32)], axis=0)
        turned = jnp.transpose(padded).astype(jnp.bfloat16)
        for i, (base, odd, way) in enumerate(places):
            at = pl.multiple_of(base + piece_row(pair * 2 + odd, way), PIECE)
            act[pl.ds(at, PIECE), :] = turned[i * PIECE:(i + 1) * PIECE]

    all_gather(b_full, 0, HALF, mlp_rows)

    def finish_out(rows, span, total):
        mixed = (state[rows, span].astype(jnp.float32) + total).astype(jnp.bfloat16)
        if last:
            own = pl.multiple_of(core * HALF + me * CHUNK + rows.start, PIECE)
            full_ref[pl.ds(own, PIECE), span] = mixed
        else:
            state_out[rows, span] = mixed

    reduce_scatter(act, down, None, finish_out)
    if last:
        all_gather(full_ref, core * HALF, core * HALF, None)
    else:
        normed_out[...] = normalise(state_out[...], next_ref)


def layer_call(call_id, layer, last, head_out, state, gain, next_gain, w_o, gate_t, up_t, w_down):
    subs = 4
    width = state.shape[-1]
    ffn = gate_t.shape[1]
    padded = 384
    vmem = pl.BlockSpec(memory_space=pltpu.VMEM)
    hbm = pl.BlockSpec(memory_space=pl.ANY)
    small = [head_out, state, gain] + ([] if last else [next_gain])
    shard = jax.ShapeDtypeStruct((CHUNK, width), jnp.bfloat16)
    outs = [jax.ShapeDtypeStruct((2 * HALF, width), jnp.bfloat16)] if last else [shard, shard]
    bf = lambda *shape: pltpu.VMEM(shape, jnp.bfloat16)
    dma = pltpu.SemaphoreType.DMA
    scratch = [bf(w_o.shape[1], width), bf(ffn, width), bf(ffn, width), bf(padded, width), bf(2 * HALF, width), bf(128, width), bf(2 * HALF, padded),
               bf(CHUNK, width), pltpu.VMEM((CHUNK, width), jnp.float32), bf(RING, CHUNK, width), bf(RING, CHUNK, width), bf(RING - 1, CHUNK, width), bf(RING - 1, CHUNK, width),
               dma((10,)), dma((RING,)), dma((RING,)), dma((14 * subs,)), dma((14 * subs,)), dma((14 * subs,)), dma((14 * subs,)), dma((16 * subs,)), dma((16 * subs,))]
    return pl.pallas_call(
        functools.partial(layer_kernel, layer, last, subs),
        out_shape=outs,
        in_specs=[vmem] * len(small) + [hbm] * 4,
        out_specs=[vmem] * len(outs),
        scratch_shapes=scratch,
        compiler_params=pltpu.CompilerParams(collective_id=call_id, has_side_effects=True, vmem_limit_bytes=60 * 1024 * 1024),
        name='layer%d' % layer,
    )(*small, w_o, gate_t, up_t, w_down)


def swap_kernel(src_ref, dst_ref, send_sem, recv_sem):
    core, me = ring_place()
    peer = (lax.axis_index('dp'), ring_device(me, 1 - core))
    barrier = pltpu.get_barrier_semaphore()
    pl.semaphore_signal(barrier, inc=1, device_id=peer, device_id_type=MESH)
    pl.semaphore_wait(barrier, 1)
    copy = pltpu.make_async_remote_copy(src_ref=src_ref, dst_ref=dst_ref, send_sem=send_sem, recv_sem=recv_sem, device_id=peer, device_id_type=MESH)
    copy.start()
    copy.wait()


def swap_call(call_id, block):
    vmem = pl.BlockSpec(memory_space=pltpu.VMEM)
    return pl.pallas_call(
        swap_kernel,
        out_shape=jax.ShapeDtypeStruct(block.shape, block.dtype),
        in_specs=[vmem],
        out_specs=vmem,
        scratch_shapes=[pltpu.SemaphoreType.DMA, pltpu.SemaphoreType.DMA],
        compiler_params=pltpu.CompilerParams(collective_id=call_id, has_side_effects=True),
        name='swap%d' % call_id,
    )(block)


def attention_kernel(block, scale, meta_ref, q_ref, r_ref, ckv_ref, kpe_ref, cnew_ref, knew_ref, out_ref):
    start = meta_ref[0] + pl.program_id(0) * block
    heads, steps = q_ref.shape[1], ckv_ref.shape[2]
    key_steps = lax.broadcasted_iota(jnp.int32, (heads, steps), 1)
    scores = []
    for j in range(block):
        q = q_ref[j]
        r = r_ref[j]
        s = lax.dot_general(q, ckv_ref[0, j], (((1,), (1,)), ((), ())), preferred_element_type=jnp.float32)
        s = s + jnp.dot(r, kpe_ref[0, j], preferred_element_type=jnp.float32)
        scores.append(s)
    probs = []
    fresh_probs = []
    for j in range(block):
        pos = meta_ref[1 + start + j]
        fresh = jnp.sum(q_ref[j].astype(jnp.float32) * cnew_ref[j:j + 1, :].astype(jnp.float32), axis=-1, keepdims=True)
        fresh = fresh + jnp.sum(r_ref[j].astype(jnp.float32) * knew_ref[j:j + 1, :].astype(jnp.float32), axis=-1, keepdims=True)
        at_pos = key_steps == pos
        s = jnp.where(at_pos, fresh, scores[j]) * scale
        s = jnp.where(key_steps <= pos, s, -jnp.inf)
        e = jnp.exp(s - jnp.max(s, axis=-1, keepdims=True))
        p = (e / jnp.sum(e, axis=-1, keepdims=True)).astype(jnp.bfloat16).astype(jnp.float32)
        fresh_probs.append(jnp.sum(jnp.where(at_pos, p, 0.0), axis=-1, keepdims=True))
        probs.append(jnp.where(at_pos, 0.0, p).astype(jnp.bfloat16))
    for j in range(block):
        c = jnp.dot(probs[j], ckv_ref[0, j], preferred_element_type=jnp.float32)
        c = c + fresh_probs[j] * cnew_ref[j:j + 1, :].astype(jnp.float32)
        out_ref[j] = c.astype(jnp.bfloat16)


def attention_call(layer, core, positions, q_lat, q_rope, ckv_cache, kpe_cache, c_new, k_new, scale):
    block = 8
    rows, heads, latent = q_lat.shape
    rope = q_rope.shape[-1]
    steps = ckv_cache.shape[2]
    meta = jnp.concatenate([jnp.reshape(core * HALF, (1,)).astype(jnp.int32), positions])
    blocks = rows // block
    grid_spec = pltpu.PrefetchScalarGridSpec(
        num_scalar_prefetch=1,
        grid=(blocks,),
        in_specs=[
            pl.BlockSpec((block, heads, latent), lambda i, m: (i, 0, 0)),
            pl.BlockSpec((block, heads, rope), lambda i, m: (i, 0, 0)),
            pl.BlockSpec((1, block, steps, latent), lambda i, m: (layer, m[0] // block + i, 0, 0)),
            pl.BlockSpec((1, block, rope, steps), lambda i, m: (layer, m[0] // block + i, 0, 0)),
            pl.BlockSpec((block, latent), lambda i, m: (i, 0)),
            pl.BlockSpec((block, rope), lambda i, m: (i, 0)),
        ],
        out_specs=pl.BlockSpec((block, heads, latent), lambda i, m: (i, 0, 0)),
    )
    return pl.pallas_call(
        functools.partial(attention_kernel, block, scale),
        out_shape=jax.ShapeDtypeStruct((rows, heads, latent), jnp.bfloat16),
        grid_spec=grid_spec,
        compiler_params=pltpu.CompilerParams(vmem_limit_bytes=32 * 1024 * 1024),
        cost_estimate=pl.CostEstimate(flops=4 * rows * heads * steps * latent, bytes_accessed=rows * steps * (latent + rope) * 2, transcendentals=rows * heads * steps),
        name='attention',
    )(meta, q_lat, q_rope, ckv_cache, kpe_cache, c_new, k_new)


def solution(mesh):
    cache_spec = P(None, 'dp', None, None)
    head_spec = P(None, None, 'tp', None)
    weight_specs = (P(), P(), P(), P(), P(), head_spec, head_spec, head_spec, P(None, 'tp', None, None), P(), P(None, None, 'tp'), P(None, None, 'tp'), P(None, 'tp', None))
    in_specs = (P('dp', None), P('dp'), cache_spec, cache_spec) + weight_specs
    out_specs = (P('dp', None), P(None, 'dp', None), P(None, 'dp', None))
    pairs = [(i, i + 1 - 2 * (i % 2)) for i in range(16)]

    def device_body(x_in, pos_ids, ckv_cache, kpe_cache, attn_gain, w_dq, q_gain, w_dkv, kv_gain, w_uq, w_uk, w_uv, w_o, mlp_gain, w_gate, w_up, w_down):
        core, me = ring_place()
        layers, latent = ckv_cache.shape[0], ckv_cache.shape[-1]
        width = x_in.shape[-1]
        nope = w_uk.shape[-1]
        lora = w_dq.shape[-1]
        scale = w_uq.shape[-1] ** -0.5
        first = core * HALF + me * CHUNK
        kpe_t = jnp.swapaxes(kpe_cache, 2, 3)
        gate_t = jnp.swapaxes(w_gate, 1, 2)
        up_t = jnp.swapaxes(w_up, 1, 2)
        w_o_flat = w_o.reshape(layers, -1, width)
        p_uq, p_uk, p_uv = [lax.ppermute(w, 'tp', pairs) for w in (w_uq, w_uk, w_uv)]
        state = lax.dynamic_slice_in_dim(x_in, first, CHUNK, 0)
        pos_rows = lax.dynamic_slice_in_dim(pos_ids, first, CHUNK, 0)
        pos_half = lax.dynamic_slice_in_dim(pos_ids, core * HALF, HALF, 0)
        c_rows = []
        k_rows = []
        for layer in range(layers):
            if layer == 0:
                normed = rms_norm(lax.dynamic_slice_in_dim(x_in, core * HALF, HALF, 0), attn_gain[0])
            own_pos = pos_half if layer == 0 else pos_rows
            c_q = rms_norm(jnp.dot(normed, w_dq[layer], preferred_element_type=jnp.float32), q_gain[layer])
            kv_lat = jnp.dot(normed, w_dkv[layer], preferred_element_type=jnp.float32)
            c_new = rms_norm(kv_lat[:, :latent], kv_gain[layer])
            k_new = rotary(kv_lat[:, latent:], own_pos).astype(jnp.bfloat16)
            if layer == 0:
                own_q, c_half, k_half = c_q, c_new, k_new
                rows = jnp.concatenate([c_new, k_new], axis=-1)
                peer_rows = lax.ppermute(rows, 'tp', pairs)
            else:
                pad = jnp.zeros((CHUNK, 192), jnp.bfloat16)
                shard = jnp.concatenate([c_q, c_new, k_new, pad], axis=-1)
                latents, = comm_call(1, False, False, True, False, 2, (shard,), shard.shape[-1])
                own_q = latents[:HALF, :lora]
                c_half, k_half = latents[:HALF, lora:lora + latent], latents[:HALF, lora + latent:lora + latent + 64]
                rows, peer_rows = latents[:HALF, lora:lora + latent + 64], latents[HALF:, lora:lora + latent + 64]
            ordered = jnp.where(core == 0, jnp.concatenate([rows, peer_rows], axis=0), jnp.concatenate([peer_rows, rows], axis=0))
            c_rows.append(ordered[:, :latent])
            k_rows.append(ordered[:, latent:])
            q_lats = []
            q_ropes = []
            for weight_q, weight_k in ((w_uq, w_uk), (p_uq, p_uk)):
                q_full = jnp.einsum('bc,chd->bhd', own_q, weight_q[layer], preferred_element_type=jnp.float32)
                q_nope = q_full[..., :nope].astype(jnp.bfloat16)
                q_ropes.append(rotary(q_full[..., nope:], pos_half[:, None]).astype(jnp.bfloat16))
                q_lats.append(jnp.einsum('bhn,chn->bhc', q_nope, weight_k[layer], preferred_element_type=jnp.float32).astype(jnp.bfloat16))
            q_lat = jnp.concatenate(q_lats, axis=1)
            q_rope = jnp.concatenate(q_ropes, axis=1)
            context = attention_call(layer, core, pos_ids, q_lat, q_rope, ckv_cache, kpe_t, c_half, k_half, scale)
            heads = w_uv.shape[2]
            own_o = jnp.einsum('bhc,chv->bhv', context[:, :heads], w_uv[layer], preferred_element_type=jnp.float32).astype(jnp.bfloat16)
            peer_o = jnp.einsum('bhc,chv->bhv', context[:, heads:], p_uv[layer], preferred_element_type=jnp.float32).astype(jnp.bfloat16)
            peer_o = swap_call(2, peer_o.reshape(HALF, -1))
            head_out = jnp.concatenate([own_o.reshape(HALF, -1), peer_o], axis=0)
            last = layer + 1 == layers
            outs = layer_call(3 + layer, layer, last, head_out, state, mlp_gain[layer][None], None if last else attn_gain[layer + 1][None], w_o_flat, gate_t, up_t, w_down)
            if last:
                x_out, = outs
            else:
                state, normed = outs
        return x_out, jnp.stack(c_rows), jnp.stack(k_rows)

    return jax.shard_map(device_body, mesh=mesh, in_specs=in_specs, out_specs=out_specs, check_vma=False)
```

```python
import functools
import math
import jax
import jax.numpy as jnp
from jax import lax
from jax.experimental import pallas as pl
from jax.experimental.pallas import tpu as pltpu
from jax.sharding import PartitionSpec as P

NORM_EPS = 1e-6
ROPE_BASE = 10000.0
MESH = pl.DeviceIdType.MESH
RING = 8
CHUNK = 32
PIECE = 16
HALF = 256


def rms_norm(values, norm_gain):
    values = values.astype(jnp.float32)
    inv_rms = lax.rsqrt(jnp.mean(values * values, axis=-1, keepdims=True) + NORM_EPS)
    return (values * inv_rms * norm_gain.astype(jnp.float32)).astype(jnp.bfloat16)


def rotary(values, positions):
    half_dim = values.shape[-1] // 2
    inv_freq = jnp.exp(jnp.arange(half_dim, dtype=jnp.float32) * (-2.0 * math.log(ROPE_BASE) / values.shape[-1]))
    angles = positions.astype(jnp.float32)[..., None] * inv_freq
    cos_part = jnp.cos(angles)
    sin_part = jnp.sin(angles)
    lo_half = values[..., :half_dim]
    hi_half = values[..., half_dim:]
    return jnp.concatenate([lo_half * cos_part - hi_half * sin_part, hi_half * cos_part + lo_half * sin_part], axis=-1)


def ring_place():
    index = lax.axis_index('tp')
    core = index % 2
    chip = index // 2
    y = chip % 2
    z = chip // 2
    return core, z * (1 - y) + (7 - z) * y


def ring_device(position, core):
    y = position // 4
    z = position * (1 - y) + (7 - position) * y
    return (z * 2 + y) * 2 + core


def comm_kernel(reduce, norm, gather, canonical, subs, *refs):
    refs = list(refs)
    if reduce:
        part_ref = refs.pop(0)
        hidden_ref = refs.pop(0)
        gain_ref = refs.pop(0) if norm else None
        state_ref = refs.pop(0) if norm else None
        normed_ref = refs.pop(0) if norm and not gather else None
    else:
        shard_ref = refs.pop(0)
    full_ref = refs.pop(0) if gather else None
    if reduce:
        pair_buf, recv_buf, send_buf, pair_send, pair_recv, rs_send, rs_recv = refs[:7]
        refs = refs[7:]
    if gather:
        ag_send, ag_recv, fw_send, fw_recv = refs[:4]
    core, me = ring_place()
    dp_index = lax.axis_index('dp')
    right = (dp_index, ring_device((me + 1) % RING, core))
    left = (dp_index, ring_device((me + RING - 1) % RING, core))
    peer = (dp_index, ring_device(me, 1 - core))
    width = (part_ref if reduce else shard_ref).shape[-1]
    cols = width // subs

    barrier = pltpu.get_barrier_semaphore()
    for other in (left, right, peer):
        pl.semaphore_signal(barrier, inc=1, device_id=other, device_id_type=MESH)
    pl.semaphore_wait(barrier, 3)

    def remote(src, dst, send, recv, target):
        copy = pltpu.make_async_remote_copy(src_ref=src, dst_ref=dst, send_sem=send, recv_sem=recv, device_id=target, device_id_type=MESH)
        copy.start()
        return copy

    pending = []
    ways = ((right, -1), (left, 1))
    if reduce:
        pair_copies = {}
        for step in range(RING):
            for way, (target, sign) in enumerate(ways):
                piece = step * 2 + way
                chunk = (me + RING + sign * (1 + step)) % RING
                row = pl.multiple_of(chunk * CHUNK + way * PIECE, PIECE)
                pair_copies[piece] = remote(part_ref.at[pl.ds(HALF + row, PIECE)], pair_buf.at[piece], pair_send.at[piece], pair_recv.at[piece], peer)
        ring_copies = {}
        for step in range(RING):
            for way, (target, sign) in enumerate(ways):
                piece = step * 2 + way
                chunk = (me + RING + sign * (1 + step)) % RING
                row = pl.multiple_of(chunk * CHUNK + way * PIECE, PIECE)
                pair_copies[piece].wait()
                for sub in range(subs):
                    span = pl.ds(sub * cols, cols)
                    total = part_ref[pl.ds(row, PIECE), span].astype(jnp.float32) + pair_buf[piece, :, span].astype(jnp.float32)
                    if step > 0:
                        before = ring_copies[step - 1, way, sub]
                        before.wait_recv()
                        pending.append(before)
                        total = total + recv_buf[(step - 1) * 2 + way, :, span].astype(jnp.float32)
                    if step < RING - 1:
                        send_buf[piece, :, span] = total.astype(jnp.bfloat16)
                        ring_copies[step, way, sub] = remote(send_buf.at[piece, :, span], recv_buf.at[piece, :, span], rs_send.at[piece * subs + sub], rs_recv.at[piece * subs + sub], target)
                    else:
                        rows = pl.ds(way * PIECE, PIECE)
                        mixed = (hidden_ref[rows, span].astype(jnp.float32) + total).astype(jnp.bfloat16)
                        if norm:
                            state_ref[rows, span] = mixed
                        else:
                            own = pl.multiple_of((core * HALF if canonical else 0) + me * CHUNK + way * PIECE, PIECE)
                            full_ref[pl.ds(own, PIECE), span] = mixed
        if norm:
            for way in range(2):
                rows = pl.ds(way * PIECE, PIECE)
                values = state_ref[rows, :].astype(jnp.float32)
                inv_rms = lax.rsqrt(jnp.mean(values * values, axis=-1, keepdims=True) + NORM_EPS)
                normed = (values * inv_rms * gain_ref[...].astype(jnp.float32)).astype(jnp.bfloat16)
                if gather:
                    own = pl.multiple_of((core * HALF if canonical else 0) + me * CHUNK + way * PIECE, PIECE)
                    full_ref[pl.ds(own, PIECE), :] = normed
                else:
                    normed_ref[rows, :] = normed
    elif gather:
        own = pl.multiple_of((core * HALF if canonical else 0) + me * CHUNK, PIECE)
        full_ref[pl.ds(own, CHUNK), :] = shard_ref[...]
    if gather:
        base_here = core * HALF if canonical else 0
        base_peer = core * HALF if canonical else HALF

        def place(base, chunk, way):
            return pl.ds(pl.multiple_of(base + chunk * CHUNK + way * PIECE, PIECE), PIECE)

        ring_copies = {}
        fw_copies = []
        for step in range(RING):
            for way, (target, sign) in enumerate(ways):
                chunk = (me + RING + sign * step) % RING
                here = place(base_here, chunk, way)
                there = place(base_peer, chunk, way)
                for sub in range(subs):
                    span = pl.ds(sub * cols, cols)
                    slot = (step * 2 + way) * subs + sub
                    if step > 0:
                        before = ring_copies[step - 1, way, sub]
                        before.wait_recv()
                        pending.append(before)
                    if step < RING - 1:
                        ring_copies[step, way, sub] = remote(full_ref.at[here, span], full_ref.at[here, span], ag_send.at[slot], ag_recv.at[slot], target)
                    fw_copies.append(remote(full_ref.at[here, span], full_ref.at[there, span], fw_send.at[slot], fw_recv.at[slot], peer))
        for copy in fw_copies:
            copy.wait()
    for copy in pending:
        copy.wait_send()


def comm_call(call_id, reduce, norm, gather, canonical, subs, operands, width):
    vmem = pl.BlockSpec(memory_space=pltpu.VMEM)
    outs = []
    if reduce and norm:
        outs.append(jax.ShapeDtypeStruct((CHUNK, width), jnp.bfloat16))
        if not gather:
            outs.append(jax.ShapeDtypeStruct((CHUNK, width), jnp.bfloat16))
    if gather:
        outs.append(jax.ShapeDtypeStruct((2 * HALF, width), jnp.bfloat16))
    scratch = []
    dma = pltpu.SemaphoreType.DMA
    if reduce:
        scratch += [pltpu.VMEM((16, PIECE, width), jnp.bfloat16), pltpu.VMEM((14, PIECE, width), jnp.bfloat16), pltpu.VMEM((14, PIECE, width), jnp.bfloat16)]
        scratch += [dma((16,)), dma((16,)), dma((14 * subs,)), dma((14 * subs,))]
    if gather:
        scratch += [dma((14 * subs,)), dma((14 * subs,)), dma((16 * subs,)), dma((16 * subs,))]
    return pl.pallas_call(
        functools.partial(comm_kernel, reduce, norm, gather, canonical, subs),
        out_shape=outs,
        in_specs=[vmem] * len(operands),
        out_specs=[vmem] * len(outs),
        scratch_shapes=scratch,
        compiler_params=pltpu.CompilerParams(collective_id=call_id, has_side_effects=True, vmem_limit_bytes=48 * 1024 * 1024),
        name='comm%d' % call_id,
    )(*operands)


def layer_kernel(layer, last, subs, scale, *refs):
    refs = list(refs)
    pos_ref, q_ref, r_ref, cnew_ref, knew_ref, wuv_ref, hidden_ref, gain_ref = refs[:8]
    refs = refs[8:]
    next_ref = None if last else refs.pop(0)
    ckv_hbm, kpe_hbm, wo_hbm, gate_hbm, up_hbm, down_hbm = refs[:6]
    refs = refs[6:]
    if last:
        full_ref = b_full = refs.pop(0)
    else:
        state_out, normed_out, b_full = refs[:3]
        refs = refs[3:]
    (ckv, kpe, o_own, o_out, o_in, wo, gate, up, down, batch, act, state, own_part, pair_out, pair_buf, recv_buf, send_buf,
     ckv_sem, kpe_sem, o_send, o_recv, w_sem, pair_send, pair_recv, rs_send, rs_recv, ag_send, ag_recv, fw_send, fw_recv) = refs
    width = hidden_ref.shape[-1]
    cols = width // subs
    block = 1024
    blocks = width // block
    ffn = gate.shape[0]
    core, me = ring_place()
    dp_index = lax.axis_index('dp')
    right = (dp_index, ring_device((me + 1) % RING, core))
    left = (dp_index, ring_device((me + RING - 1) % RING, core))
    peer = (dp_index, ring_device(me, 1 - core))
    ways = ((right, -1), (left, 1))

    def wo_copy(i):
        span = pl.ds(pl.multiple_of(i * block, block), block)
        return pltpu.make_async_copy(wo_hbm.at[layer, :, span], wo.at[:, span], w_sem.at[i])

    gate_copy = pltpu.make_async_copy(gate_hbm.at[layer], gate, w_sem.at[blocks])
    up_copy = pltpu.make_async_copy(up_hbm.at[layer], up, w_sem.at[blocks + 1])
    down_copy = pltpu.make_async_copy(down_hbm.at[layer], down.at[pl.ds(0, ffn)], w_sem.at[blocks + 2])
    seqs = ckv.shape[1]
    quarters = CHUNK // seqs

    def seq_row(step, k):
        way, part = divmod(k, quarters // 2)
        return pl.multiple_of(piece_row(step + 1, way) + part * seqs, seqs)

    def cache_copies(step, k):
        at = pl.ds(pl.multiple_of(core * HALF + seq_row(step, k), seqs), seqs)
        return (pltpu.make_async_copy(ckv_hbm.at[layer, at], ckv.at[k], ckv_sem.at[k]), pltpu.make_async_copy(kpe_hbm.at[layer, at], kpe.at[k], kpe_sem.at[k]))

    def piece_row(step, way):
        chunk = (me + RING + (step if way else -step)) % RING
        return pl.multiple_of(chunk * CHUNK + way * PIECE, PIECE)

    for k in range(quarters):
        for copy in cache_copies(0, k):
            copy.start()
    for i in range(blocks):
        wo_copy(i).start()
    gate_copy.start()
    up_copy.start()
    down_copy.start()

    barrier = pltpu.get_barrier_semaphore()
    for other in (left, right, peer):
        pl.semaphore_signal(barrier, inc=1, device_id=other, device_id_type=MESH)
    pl.semaphore_wait(barrier, 3)

    def remote(src, dst, send, recv, target):
        return pltpu.make_async_remote_copy(src_ref=src, dst_ref=dst, send_sem=send, recv_sem=recv, device_id=target, device_id_type=MESH)

    def o_copy(step):
        return remote(o_out.at[step], o_in.at[step], o_send.at[step], o_recv.at[step], peer)

    def attend(step):
        heads, steps = q_ref.shape[1], ckv.shape[2]
        value = wuv_ref.shape[1] // heads
        mine = o_own.shape[-1]
        key_steps = lax.broadcasted_iota(jnp.int32, (heads, steps), 1)
        row_head = lax.broadcasted_iota(jnp.int32, (seqs, heads, wuv_ref.shape[1]), 1)
        col_head = lax.broadcasted_iota(jnp.int32, (seqs, heads, wuv_ref.shape[1]), 2) // value

        def score(k):
            row = seq_row(step, k)
            for copy in cache_copies(step, k):
                copy.wait()
            scores = []
            for j in range(seqs):
                s = lax.dot_general(q_ref[row + j], ckv[k, j], (((1,), (1,)), ((), ())), preferred_element_type=jnp.float32)
                scores.append(s + jnp.dot(r_ref[row + j], kpe[k, j], preferred_element_type=jnp.float32))
            return scores

        def weigh(k, scores):
            row = seq_row(step, k)
            c_new = cnew_ref[pl.ds(row, seqs), :].astype(jnp.float32)
            k_new = knew_ref[pl.ds(row, seqs), :].astype(jnp.float32)
            context = []
            for j in range(seqs):
                pos = pos_ref[core * HALF + row + j]
                fresh = jnp.sum(q_ref[row + j].astype(jnp.float32) * c_new[j:j + 1], axis=-1, keepdims=True)
                fresh = fresh + jnp.sum(r_ref[row + j].astype(jnp.float32) * k_new[j:j + 1], axis=-1, keepdims=True)
                at_pos = key_steps == pos
                s = jnp.where(at_pos, fresh, scores[j]) * scale
                s = jnp.where(key_steps <= pos, s, -jnp.inf)
                e = jnp.exp(s - jnp.max(s, axis=-1, keepdims=True))
                p = (e / jnp.sum(e, axis=-1, keepdims=True)).astype(jnp.bfloat16).astype(jnp.float32)
                fresh_prob = jnp.sum(jnp.where(at_pos, p, 0.0), axis=-1, keepdims=True)
                c = jnp.dot(jnp.where(at_pos, 0.0, p).astype(jnp.bfloat16), ckv[k, j], preferred_element_type=jnp.float32)
                context.append((c + fresh_prob * c_new[j:j + 1]).astype(jnp.bfloat16))
            spread = jnp.dot(jnp.concatenate(context, axis=0), wuv_ref[...], preferred_element_type=jnp.float32)
            spread = spread.reshape(seqs, heads, wuv_ref.shape[1])
            out = jnp.sum(jnp.where(row_head == col_head, spread, 0.0), axis=1).astype(jnp.bfloat16)
            o_own[step, pl.ds(k * seqs, seqs), :] = out[:, :mine]
            o_out[step, pl.ds(k * seqs, seqs), :] = out[:, mine:]
            for copy in cache_copies((step + 1) % RING, k):
                copy.start()

        scores = score(0)
        for k in range(quarters):
            later = score(k + 1) if k + 1 < quarters else None
            weigh(k, scores)
            scores = later
        o_copy(step).start()

    def pair_copy(step):
        return remote(pair_out.at[step], pair_buf.at[step], pair_send.at[step], pair_recv.at[step], peer)

    def rs_copy(step, way, sub):
        slot = (step * 2 + way) * subs + sub
        where = (step, pl.ds(way * PIECE, PIECE), pl.ds(sub * cols, cols))
        return remote(send_buf.at[where], recv_buf.at[where], rs_send.at[slot], rs_recv.at[slot], ways[way][0])

    def reduce_scatter(attention, weight, ready, finish):
        def multiply(step):
            if attention:
                o_copy(step).wait_recv()
                lhs = jnp.concatenate([o_own[step], o_in[step]], axis=0)
            else:
                near, far = piece_row(step + 1, 0), piece_row(step + 1, 1)
                lhs = jnp.concatenate([act[pl.ds(pl.multiple_of(base + at, PIECE), PIECE), :] for base in (0, HALF) for at in (near, far)], axis=0)

            def one_block(i, carry):
                span = pl.ds(pl.multiple_of(i * block, block), block)
                if ready is not None:
                    @pl.when(step == 0)
                    def _():
                        ready(i)
                prod = jnp.dot(lhs, weight[:, span], preferred_element_type=jnp.float32)
                own_part[step % 2, :, span] = prod[:CHUNK]
                pair_out[step, :, span] = prod[CHUNK:].astype(jnp.bfloat16)
                return carry

            lax.fori_loop(0, blocks, one_block, 0)
            pair_copy(step).start()

        def pass_on(step):
            pair_copy(step).wait_recv()
            for sub in range(subs):
                span = pl.ds(sub * cols, cols)
                for way in range(2):
                    rows = pl.ds(way * PIECE, PIECE)

                    @pl.when(step > 0)
                    def _():
                        rs_copy(step - 1, way, sub).wait_recv()
                        own_part[step % 2, rows, span] += recv_buf[step - 1, rows, span].astype(jnp.float32)

                    total = own_part[step % 2, rows, span] + pair_buf[step, rows, span].astype(jnp.float32)

                    @pl.when(step < RING - 1)
                    def _():
                        send_buf[step, rows, span] = total.astype(jnp.bfloat16)
                        rs_copy(step, way, sub).start()

                    @pl.when(step == RING - 1)
                    def _():
                        finish(rows, span, total)

        def staggered(i, carry):
            if attention:
                @pl.when(i < RING)
                def _():
                    attend(i)

                @pl.when(i > 1)
                def _():
                    pass_on(i - 2)

                @pl.when((i > 0) & (i <= RING))
                def _():
                    multiply(i - 1)
            else:
                @pl.when(i < RING)
                def _():
                    multiply(i)

                @pl.when(i > 0)
                def _():
                    pass_on(i - 1)
            return carry

        lax.fori_loop(0, RING + (2 if attention else 1), staggered, 0)
        if attention:
            for k in range(quarters):
                for copy in cache_copies(0, k):
                    copy.wait()

        def drain(step, carry):
            pair_copy(step).wait_send()
            if attention:
                o_copy(step).wait_send()

            @pl.when(step < RING - 1)
            def _():
                for way in range(2):
                    for sub in range(subs):
                        rs_copy(step, way, sub).wait_send()
            return carry

        lax.fori_loop(0, RING, drain, 0)

    def normalise(values, gain):
        values = values.astype(jnp.float32)
        inv_rms = lax.rsqrt(jnp.mean(values * values, axis=-1, keepdims=True) + NORM_EPS)
        return (values * inv_rms * gain[...].astype(jnp.float32)).astype(jnp.bfloat16)

    def all_gather(buf, base_here, base_there, consume):
        def ag_copy(step, way, sub):
            slot = (step * 2 + way) * subs + sub
            here = buf.at[pl.ds(pl.multiple_of(base_here + piece_row(step, way), PIECE), PIECE), pl.ds(sub * cols, cols)]
            return remote(here, here, ag_send.at[slot], ag_recv.at[slot], ways[way][0])

        def fw_copy(step, way, sub):
            slot = (step * 2 + way) * subs + sub
            here = buf.at[pl.ds(pl.multiple_of(base_here + piece_row(step, way), PIECE), PIECE), pl.ds(sub * cols, cols)]
            there = buf.at[pl.ds(pl.multiple_of(base_there + piece_row(step, way), PIECE), PIECE), pl.ds(sub * cols, cols)]
            return remote(here, there, fw_send.at[slot], fw_recv.at[slot], peer)

        def two_steps(pair, carry):
            for odd in range(2):
                step = pair * 2 + odd
                for sub in range(subs):
                    for way in range(2):
                        if odd:
                            ag_copy(step - 1, way, sub).wait_recv()
                        else:
                            @pl.when(pair > 0)
                            def _():
                                ag_copy(step - 1, way, sub).wait_recv()
                        if odd:
                            @pl.when(pair < RING // 2 - 1)
                            def _():
                                ag_copy(step, way, sub).start()
                        else:
                            ag_copy(step, way, sub).start()
                        fw_copy(step, way, sub).start()
            for odd in range(2):
                for way in range(2):
                    for sub in range(subs):
                        fw_copy(pair * 2 + odd, way, sub).wait_recv()
            if consume is not None:
                consume(pair)
            return carry

        lax.fori_loop(0, RING // 2, two_steps, 0)

        def drain(step, carry):
            for way in range(2):
                for sub in range(subs):
                    fw_copy(step, way, sub).wait_send()

                    @pl.when(step < RING - 1)
                    def _():
                        ag_copy(step, way, sub).wait_send()
            return carry

        lax.fori_loop(0, RING, drain, 0)

    def finish_mid(rows, span, total):
        state[rows, span] = (hidden_ref[rows, span].astype(jnp.float32) + total).astype(jnp.bfloat16)

    reduce_scatter(True, wo, lambda i: wo_copy(i).wait(), finish_mid)
    b_full[pl.ds(pl.multiple_of(me * CHUNK, CHUNK), CHUNK), :] = normalise(state[...], gain_ref)
    down[pl.ds(ffn, down.shape[0] - ffn), :] = jnp.zeros((down.shape[0] - ffn, width), jnp.bfloat16)
    gate_copy.wait()
    up_copy.wait()
    down_copy.wait()

    def mlp_rows(pair):
        places = [(base, step, way) for base in (0, HALF) for step in range(2) for way in range(2)]
        for i, (base, odd, way) in enumerate(places):
            at = pl.multiple_of(base + piece_row(pair * 2 + odd, way), PIECE)
            batch[pl.ds(i * PIECE, PIECE), :] = b_full[pl.ds(at, PIECE), :]
        dims = (((1,), (1,)), ((), ()))
        gate_pre = lax.dot_general(gate[...], batch[...], dims, preferred_element_type=jnp.float32)
        up_pre = lax.dot_general(up[...], batch[...], dims, preferred_element_type=jnp.float32)
        hidden_act = jax.nn.silu(gate_pre) * up_pre
        padded = jnp.concatenate([hidden_act, jnp.zeros((act.shape[1] - ffn, 128), jnp.float32)], axis=0)
        turned = jnp.transpose(padded).astype(jnp.bfloat16)
        for i, (base, odd, way) in enumerate(places):
            at = pl.multiple_of(base + piece_row(pair * 2 + odd, way), PIECE)
            act[pl.ds(at, PIECE), :] = turned[i * PIECE:(i + 1) * PIECE]

    all_gather(b_full, 0, HALF, mlp_rows)

    def finish_out(rows, span, total):
        mixed = (state[rows, span].astype(jnp.float32) + total).astype(jnp.bfloat16)
        if last:
            own = pl.multiple_of(core * HALF + me * CHUNK + rows.start, PIECE)
            full_ref[pl.ds(own, PIECE), span] = mixed
        else:
            state_out[rows, span] = mixed

    reduce_scatter(False, down, None, finish_out)
    if last:
        all_gather(full_ref, core * HALF, core * HALF, None)
    else:
        normed_out[...] = normalise(state_out[...], next_ref)


def layer_call(call_id, layer, last, positions, q_lat, q_rope, c_new, k_new, w_uv, ckv_cache, kpe_cache, state, gain, next_gain, w_o, gate_t, up_t, w_down, scale):
    subs = 4
    seqs = 8
    width = state.shape[-1]
    ffn = gate_t.shape[1]
    padded = 384
    vmem = pl.BlockSpec(memory_space=pltpu.VMEM)
    hbm = pl.BlockSpec(memory_space=pl.ANY)
    small = [q_lat, q_rope, c_new, k_new, w_uv, state, gain] + ([] if last else [next_gain])
    shard = jax.ShapeDtypeStruct((CHUNK, width), jnp.bfloat16)
    outs = [jax.ShapeDtypeStruct((2 * HALF, width), jnp.bfloat16)] if last else [shard, shard]
    bf = lambda *shape: pltpu.VMEM(shape, jnp.bfloat16)
    dma = pltpu.SemaphoreType.DMA
    quarters = CHUNK // seqs
    mine = w_o.shape[1]
    scratch = ([] if last else [bf(2 * HALF, width)]) + [
        bf(quarters, seqs, *ckv_cache.shape[2:]), bf(quarters, seqs, *kpe_cache.shape[2:]), bf(RING, CHUNK, mine), bf(RING, CHUNK, mine), bf(RING, CHUNK, mine),
        bf(mine, width), bf(ffn, width), bf(ffn, width), bf(padded, width), bf(128, width), bf(2 * HALF, padded),
        bf(CHUNK, width), pltpu.VMEM((2, CHUNK, width), jnp.float32), bf(RING, CHUNK, width), bf(RING, CHUNK, width), bf(RING - 1, CHUNK, width), bf(RING - 1, CHUNK, width),
        dma((quarters,)), dma((quarters,)), dma((RING,)), dma((RING,)), dma((10,)), dma((RING,)), dma((RING,)),
        dma((14 * subs,)), dma((14 * subs,)), dma((14 * subs,)), dma((14 * subs,)), dma((16 * subs,)), dma((16 * subs,))]
    return pl.pallas_call(
        functools.partial(layer_kernel, layer, last, subs, scale),
        out_shape=outs,
        in_specs=[pl.BlockSpec(memory_space=pltpu.SMEM)] + [vmem] * len(small) + [hbm] * 6,
        out_specs=[vmem] * len(outs),
        scratch_shapes=scratch,
        compiler_params=pltpu.CompilerParams(collective_id=call_id, has_side_effects=True, vmem_limit_bytes=67043328),
        name='layer%d' % layer,
    )(positions, *small, ckv_cache, kpe_cache, w_o, gate_t, up_t, w_down)


def query_kernel(c_ref, cos_ref, sin_ref, own_q, peer_q, wk_ref, u_ref, r_ref):
    both_last = (((1,), (1,)), ((), ()))
    nope = wk_ref.shape[2]
    half = cos_ref.shape[1]
    for group, weight in enumerate((own_q, peer_q)):
        for h in range(weight.shape[1]):
            head = group * weight.shape[1] + h
            q = lax.dot_general(c_ref[...], weight[0, h], both_last, preferred_element_type=jnp.float32)
            lo, hi = q[:, nope:nope + half], q[:, nope + half:]
            r_ref[head] = jnp.concatenate([lo * cos_ref[...] - hi * sin_ref[...], hi * cos_ref[...] + lo * sin_ref[...]], axis=-1).astype(jnp.bfloat16)
            u_ref[head] = lax.dot_general(q[:, :nope].astype(jnp.bfloat16), wk_ref[head], both_last, preferred_element_type=jnp.float32).astype(jnp.bfloat16)


def query_call(layer, c_q, cos_part, sin_part, own_q, peer_q, w_k):
    rows = c_q.shape[0]
    heads, latent = w_k.shape[0], w_k.shape[1]
    rope = 2 * cos_part.shape[1]
    whole = lambda x: pl.BlockSpec(x.shape, lambda i: (0,) * x.ndim)
    picked = lambda x: pl.BlockSpec((1,) + x.shape[1:], lambda i: (layer, 0, 0, 0))
    outs = [jax.ShapeDtypeStruct((heads, rows, latent), jnp.bfloat16), jax.ShapeDtypeStruct((heads, rows, rope), jnp.bfloat16)]
    return pl.pallas_call(
        query_kernel,
        out_shape=outs,
        grid=(1,),
        in_specs=[whole(c_q), whole(cos_part), whole(sin_part), picked(own_q), picked(peer_q), whole(w_k)],
        out_specs=[whole(outs[0]), whole(outs[1])],
        cost_estimate=pl.CostEstimate(flops=2 * rows * c_q.shape[1] * heads * 192, bytes_accessed=8 * 1024 * 1024, transcendentals=0),
        name='queries',
    )(c_q, cos_part, sin_part, own_q, peer_q, w_k)


def solution(mesh):
    cache_spec = P(None, 'dp', None, None)
    head_spec = P(None, None, 'tp', None)
    weight_specs = (P(), P(), P(), P(), P(), head_spec, head_spec, head_spec, P(None, 'tp', None, None), P(), P(None, None, 'tp'), P(None, None, 'tp'), P(None, 'tp', None))
    in_specs = (P('dp', None), P('dp'), cache_spec, cache_spec) + weight_specs
    out_specs = (P('dp', None), P(None, 'dp', None), P(None, 'dp', None))
    pairs = [(i, i + 1 - 2 * (i % 2)) for i in range(16)]

    def device_body(x_in, pos_ids, ckv_cache, kpe_cache, attn_gain, w_dq, q_gain, w_dkv, kv_gain, w_uq, w_uk, w_uv, w_o, mlp_gain, w_gate, w_up, w_down):
        core, me = ring_place()
        layers, latent = ckv_cache.shape[0], ckv_cache.shape[-1]
        width = x_in.shape[-1]
        nope = w_uk.shape[-1]
        lora = w_dq.shape[-1]
        scale = w_uq.shape[-1] ** -0.5
        first = core * HALF + me * CHUNK
        kpe_t = jnp.swapaxes(kpe_cache, 2, 3)
        gate_t = jnp.swapaxes(w_gate, 1, 2)
        up_t = jnp.swapaxes(w_up, 1, 2)
        w_o_flat = w_o.reshape(layers, -1, width)
        uq_t = jnp.transpose(w_uq, (0, 2, 3, 1))
        uk_t = jnp.transpose(w_uk, (0, 2, 1, 3))
        uv_t = jnp.transpose(w_uv, (0, 2, 1, 3))
        p_uq, p_uk, p_uv = [lax.ppermute(w, 'tp', pairs) for w in (uq_t, uk_t, uv_t)]
        state = lax.dynamic_slice_in_dim(x_in, first, CHUNK, 0)
        pos_rows = lax.dynamic_slice_in_dim(pos_ids, first, CHUNK, 0)
        pos_half = lax.dynamic_slice_in_dim(pos_ids, core * HALF, HALF, 0)
        half_rope = kpe_cache.shape[-1] // 2
        inv_freq = jnp.exp(jnp.arange(half_rope, dtype=jnp.float32) * (-math.log(ROPE_BASE) / half_rope))
        angles = pos_half.astype(jnp.float32)[:, None] * inv_freq
        cos_half, sin_half = jnp.cos(angles), jnp.sin(angles)
        c_rows = []
        k_rows = []
        for layer in range(layers):
            if layer == 0:
                normed = rms_norm(lax.dynamic_slice_in_dim(x_in, core * HALF, HALF, 0), attn_gain[0])
            own_pos = pos_half if layer == 0 else pos_rows
            c_q = rms_norm(jnp.dot(normed, w_dq[layer], preferred_element_type=jnp.float32), q_gain[layer])
            kv_lat = jnp.dot(normed, w_dkv[layer], preferred_element_type=jnp.float32)
            c_new = rms_norm(kv_lat[:, :latent], kv_gain[layer])
            k_new = rotary(kv_lat[:, latent:], own_pos).astype(jnp.bfloat16)
            if layer == 0:
                own_q, c_half, k_half = c_q, c_new, k_new
                rows = jnp.concatenate([c_new, k_new], axis=-1)
                peer_rows = lax.ppermute(rows, 'tp', pairs)
            else:
                pad = jnp.zeros((CHUNK, 192), jnp.bfloat16)
                shard = jnp.concatenate([c_q, c_new, k_new, pad], axis=-1)
                latents, = comm_call(1, False, False, True, False, 2, (shard,), shard.shape[-1])
                own_q = latents[:HALF, :lora]
                c_half, k_half = latents[:HALF, lora:lora + latent], latents[:HALF, lora + latent:lora + latent + 64]
                rows, peer_rows = latents[:HALF, lora:lora + latent + 64], latents[HALF:, lora:lora + latent + 64]
            ordered = jnp.where(core == 0, jnp.concatenate([rows, peer_rows], axis=0), jnp.concatenate([peer_rows, rows], axis=0))
            c_rows.append(ordered[:, :latent])
            k_rows.append(ordered[:, latent:])
            w_k = jnp.concatenate([uk_t[layer], p_uk[layer]], axis=0)
            q_lat, q_rope = query_call(layer, own_q, cos_half, sin_half, uq_t, p_uq, w_k)
            q_lat, q_rope = jnp.transpose(q_lat, (1, 0, 2)), jnp.transpose(q_rope, (1, 0, 2))
            values = jnp.transpose(jnp.concatenate([uv_t[layer], p_uv[layer]], axis=0), (1, 0, 2)).reshape(latent, -1)
            last = layer + 1 == layers
            outs = layer_call(3 + layer, layer, last, pos_ids, q_lat, q_rope, c_half, k_half, values, ckv_cache, kpe_t, state, mlp_gain[layer][None],
                              None if last else attn_gain[layer + 1][None], w_o_flat, gate_t, up_t, w_down, scale)
            if last:
                x_out, = outs
            else:
                state, normed = outs
        return x_out, jnp.stack(c_rows), jnp.stack(k_rows)

    return jax.shard_map(device_body, mesh=mesh, in_specs=in_specs, out_specs=out_specs, check_vma=False)
```

```python
import functools
import math
import jax
import jax.numpy as jnp
from jax import lax
from jax.experimental import pallas as pl
from jax.experimental.pallas import tpu as pltpu
from jax.sharding import PartitionSpec as P

NORM_EPS = 1e-6
ROPE_BASE = 10000.0
MESH = pl.DeviceIdType.MESH
RING = 8
CHUNK = 32
PIECE = 16
HALF = 256


def rms_norm(values, norm_gain):
    values = values.astype(jnp.float32)
    inv_rms = lax.rsqrt(jnp.mean(values * values, axis=-1, keepdims=True) + NORM_EPS)
    return (values * inv_rms * norm_gain.astype(jnp.float32)).astype(jnp.bfloat16)


def rotary(values, positions):
    half_dim = values.shape[-1] // 2
    inv_freq = jnp.exp(jnp.arange(half_dim, dtype=jnp.float32) * (-2.0 * math.log(ROPE_BASE) / values.shape[-1]))
    angles = positions.astype(jnp.float32)[..., None] * inv_freq
    cos_part = jnp.cos(angles)
    sin_part = jnp.sin(angles)
    lo_half = values[..., :half_dim]
    hi_half = values[..., half_dim:]
    return jnp.concatenate([lo_half * cos_part - hi_half * sin_part, hi_half * cos_part + lo_half * sin_part], axis=-1)


def ring_place():
    index = lax.axis_index('tp')
    core = index % 2
    chip = index // 2
    y = chip % 2
    z = chip // 2
    return core, z * (1 - y) + (7 - z) * y


def ring_device(position, core):
    y = position // 4
    z = position * (1 - y) + (7 - position) * y
    return (z * 2 + y) * 2 + core


def gather_kernel(shard_ref, full_ref, ag_send, ag_recv, fw_send, fw_recv):
    core, me = ring_place()
    dp_index = lax.axis_index('dp')
    right = (dp_index, ring_device((me + 1) % RING, core))
    left = (dp_index, ring_device((me + RING - 1) % RING, core))
    peer = (dp_index, ring_device(me, 1 - core))
    barrier = pltpu.get_barrier_semaphore()
    for other in (left, right, peer):
        pl.semaphore_signal(barrier, inc=1, device_id=other, device_id_type=MESH)
    full_ref[pl.ds(pl.multiple_of(me * CHUNK, CHUNK), CHUNK), :] = shard_ref[...]
    pl.semaphore_wait(barrier, 3)
    ring = {}
    handed = []
    for step in range(5):
        for sub in range(2):
            for way, (target, sign, limit) in enumerate(((right, -1, 4), (left, 1, 3))):
                if step > limit:
                    continue
                chunk = (me + RING + sign * step) % RING
                row = pl.multiple_of(chunk * CHUNK + sub * PIECE, PIECE)
                here = full_ref.at[pl.ds(row, PIECE)]
                slot = (step * 2 + way) * 2 + sub
                if step > 0:
                    ring[step - 1, way, sub].wait_recv()
                if step < limit:
                    ring[step, way, sub] = pltpu.make_async_remote_copy(src_ref=here, dst_ref=here, send_sem=ag_send.at[slot], recv_sem=ag_recv.at[slot], device_id=target, device_id_type=MESH)
                    ring[step, way, sub].start()
                if step > 0 or way == 0:
                    there = full_ref.at[pl.ds(pl.multiple_of(HALF + row, PIECE), PIECE)]
                    copy = pltpu.make_async_remote_copy(src_ref=here, dst_ref=there, send_sem=fw_send.at[slot], recv_sem=fw_recv.at[slot], device_id=peer, device_id_type=MESH)
                    copy.start()
                    handed.append(copy)
    for copy in handed:
        copy.wait()
    for copy in ring.values():
        copy.wait_send()


def gather_call(shard):
    vmem = pl.BlockSpec(memory_space=pltpu.VMEM)
    dma = pltpu.SemaphoreType.DMA
    return pl.pallas_call(
        gather_kernel,
        out_shape=jax.ShapeDtypeStruct((2 * HALF, shard.shape[-1]), shard.dtype),
        in_specs=[vmem],
        out_specs=vmem,
        scratch_shapes=[dma((16,)), dma((16,)), dma((20,)), dma((20,))],
        compiler_params=pltpu.CompilerParams(collective_id=1, has_side_effects=True, vmem_limit_bytes=8 * 1024 * 1024),
        name='gather',
    )(shard)


def layer_kernel(layer, last, subs, scale, *refs):
    refs = list(refs)
    pos_ref, q_ref, r_ref, cnew_ref, knew_ref, wuv_ref, hidden_ref, gain_ref = refs[:8]
    refs = refs[8:]
    next_ref = None if last else refs.pop(0)
    ckv_hbm, kpe_hbm, wo_hbm, gate_hbm, up_hbm, down_hbm = refs[:6]
    refs = refs[6:]
    if last:
        full_ref = b_full = refs.pop(0)
    else:
        state_out, normed_out, b_full = refs[:3]
        refs = refs[3:]
    (ckv, kpe, o_own, o_out, o_in, wo, gate, up, down, batch, gate_pre, up_pre, act, state, own_part, pair_out, pair_buf, recv_buf, send_buf,
     ckv_sem, kpe_sem, o_send, o_recv, w_sem, pair_send, pair_recv, rs_send, rs_recv, ag_send, ag_recv, fw_send, fw_recv) = refs
    width = hidden_ref.shape[-1]
    cols = width // subs
    block = 1024
    blocks = width // block
    ffn = gate.shape[0]
    core, me = ring_place()
    dp_index = lax.axis_index('dp')
    right = (dp_index, ring_device((me + 1) % RING, core))
    left = (dp_index, ring_device((me + RING - 1) % RING, core))
    peer = (dp_index, ring_device(me, 1 - core))
    ways = ((right, -1), (left, 1))

    def wo_copy(i):
        span = pl.ds(pl.multiple_of(i * block, block), block)
        return pltpu.make_async_copy(wo_hbm.at[layer, :, span], wo.at[:, span], w_sem.at[i])

    gate_copy = pltpu.make_async_copy(gate_hbm.at[layer], gate, w_sem.at[blocks])
    up_copy = pltpu.make_async_copy(up_hbm.at[layer], up, w_sem.at[blocks + 1])
    down_copy = pltpu.make_async_copy(down_hbm.at[layer], down.at[pl.ds(0, ffn)], w_sem.at[blocks + 2])
    seqs = ckv.shape[1]
    quarters = CHUNK // seqs

    def seq_row(step, k):
        way, part = divmod(k, quarters // 2)
        return pl.multiple_of(piece_row(step + 1, way) + part * seqs, seqs)

    def cache_copies(step, k):
        at = pl.ds(pl.multiple_of(core * HALF + seq_row(step, k), seqs), seqs)
        return (pltpu.make_async_copy(ckv_hbm.at[layer, at], ckv.at[k], ckv_sem.at[k]), pltpu.make_async_copy(kpe_hbm.at[layer, at], kpe.at[k], kpe_sem.at[k]))

    def piece_row(step, way):
        chunk = (me + RING + (step if way else -step)) % RING
        return pl.multiple_of(chunk * CHUNK + way * PIECE, PIECE)

    for k in range(quarters):
        for copy in cache_copies(0, k):
            copy.start()
    for i in range(blocks):
        wo_copy(i).start()
    gate_copy.start()
    up_copy.start()
    down_copy.start()

    barrier = pltpu.get_barrier_semaphore()
    for other in (left, right, peer):
        pl.semaphore_signal(barrier, inc=1, device_id=other, device_id_type=MESH)
    pl.semaphore_wait(barrier, 3)

    def remote(src, dst, send, recv, target):
        return pltpu.make_async_remote_copy(src_ref=src, dst_ref=dst, send_sem=send, recv_sem=recv, device_id=target, device_id_type=MESH)

    def o_copy(step):
        return remote(o_out.at[step], o_in.at[step], o_send.at[step], o_recv.at[step], peer)

    def attend(step):
        heads, steps = q_ref.shape[1], ckv.shape[2]
        value = wuv_ref.shape[1] // heads
        mine = o_own.shape[-1]
        key_steps = lax.broadcasted_iota(jnp.int32, (heads, steps), 1)
        row_head = lax.broadcasted_iota(jnp.int32, (seqs, heads, wuv_ref.shape[1]), 1)
        col_head = lax.broadcasted_iota(jnp.int32, (seqs, heads, wuv_ref.shape[1]), 2) // value

        def score(k):
            row = seq_row(step, k)
            for copy in cache_copies(step, k):
                copy.wait()
            scores = []
            for j in range(seqs):
                s = lax.dot_general(q_ref[row + j], ckv[k, j], (((1,), (1,)), ((), ())), preferred_element_type=jnp.float32)
                scores.append(s + jnp.dot(r_ref[row + j], kpe[k, j], preferred_element_type=jnp.float32))
            return scores

        def weigh(k, scores):
            row = seq_row(step, k)
            c_new = cnew_ref[pl.ds(row, seqs), :].astype(jnp.float32)
            k_new = knew_ref[pl.ds(row, seqs), :].astype(jnp.float32)
            context = []
            for j in range(seqs):
                pos = pos_ref[core * HALF + row + j]
                fresh = jnp.sum(q_ref[row + j].astype(jnp.float32) * c_new[j:j + 1], axis=-1, keepdims=True)
                fresh = fresh + jnp.sum(r_ref[row + j].astype(jnp.float32) * k_new[j:j + 1], axis=-1, keepdims=True)
                at_pos = key_steps == pos
                s = jnp.where(at_pos, fresh, scores[j]) * scale
                s = jnp.where(key_steps <= pos, s, -jnp.inf)
                e = jnp.exp(s - jnp.max(s, axis=-1, keepdims=True))
                p = (e / jnp.sum(e, axis=-1, keepdims=True)).astype(jnp.bfloat16).astype(jnp.float32)
                fresh_prob = jnp.sum(jnp.where(at_pos, p, 0.0), axis=-1, keepdims=True)
                c = jnp.dot(jnp.where(at_pos, 0.0, p).astype(jnp.bfloat16), ckv[k, j], preferred_element_type=jnp.float32)
                context.append((c + fresh_prob * c_new[j:j + 1]).astype(jnp.bfloat16))
            spread = jnp.dot(jnp.concatenate(context, axis=0), wuv_ref[...], preferred_element_type=jnp.float32)
            spread = spread.reshape(seqs, heads, wuv_ref.shape[1])
            out = jnp.sum(jnp.where(row_head == col_head, spread, 0.0), axis=1).astype(jnp.bfloat16)
            o_own[step, pl.ds(k * seqs, seqs), :] = out[:, :mine]
            o_out[step, pl.ds(k * seqs, seqs), :] = out[:, mine:]
            for copy in cache_copies((step + 1) % RING, k):
                copy.start()

        scores = score(0)
        for k in range(quarters):
            later = score(k + 1) if k + 1 < quarters else None
            weigh(k, scores)
            scores = later
        o_copy(step).start()

    def pair_copy(step):
        return remote(pair_out.at[step], pair_buf.at[step], pair_send.at[step], pair_recv.at[step], peer)

    def rs_copy(step, way, sub):
        slot = (step * 2 + way) * subs + sub
        where = (step, pl.ds(way * PIECE, PIECE), pl.ds(sub * cols, cols))
        return remote(send_buf.at[where], recv_buf.at[where], rs_send.at[slot], rs_recv.at[slot], ways[way][0])

    def reduce_scatter(attention, weight, ready, finish):
        per_sub = -(-blocks // subs)

        def multiply(step, sub):
            if attention:
                if sub == 0:
                    o_copy(step).wait_recv()
                lhs = jnp.concatenate([o_own[step], o_in[step]], axis=0)
            else:
                near, far = piece_row(step + 1, 0), piece_row(step + 1, 1)
                lhs = jnp.concatenate([act[pl.ds(pl.multiple_of(base + at, PIECE), PIECE), :] for base in (0, HALF) for at in (near, far)], axis=0)
            for i in range(sub * per_sub, min((sub + 1) * per_sub, blocks)):
                span = pl.ds(i * block, block)
                if ready is not None:
                    @pl.when(step == 0)
                    def _():
                        ready(i)
                prod = jnp.dot(lhs, weight[:, span], preferred_element_type=jnp.float32)
                own_part[step % 2, :, span] = prod[:CHUNK]
                pair_out[step, :, span] = prod[CHUNK:].astype(jnp.bfloat16)
            if sub == subs - 1:
                pair_copy(step).start()

        def pass_on(step, sub):
            if sub == 0:
                pair_copy(step).wait_recv()
            span = pl.ds(sub * cols, cols)
            for way in range(2):
                rows = pl.ds(way * PIECE, PIECE)

                @pl.when(step > 0)
                def _():
                    rs_copy(step - 1, way, sub).wait_recv()
                    own_part[step % 2, rows, span] += recv_buf[step - 1, rows, span].astype(jnp.float32)

                total = own_part[step % 2, rows, span] + pair_buf[step, rows, span].astype(jnp.float32)

                @pl.when(step < RING - 1)
                def _():
                    send_buf[step, rows, span] = total.astype(jnp.bfloat16)
                    rs_copy(step, way, sub).start()

                @pl.when(step == RING - 1)
                def _():
                    finish(rows, span, total)

        lag = 1 if attention else 0

        def staggered(i, carry):
            if attention:
                @pl.when(i < RING)
                def _():
                    attend(i)
            for sub in range(subs):
                @pl.when((i >= lag) & (i < RING + lag))
                def _():
                    multiply(i - lag, sub)

                @pl.when(i > lag)
                def _():
                    pass_on(i - lag - 1, sub)
            return carry

        lax.fori_loop(0, RING + 1 + lag, staggered, 0)
        if attention:
            for k in range(quarters):
                for copy in cache_copies(0, k):
                    copy.wait()

        def drain(step, carry):
            pair_copy(step).wait_send()
            if attention:
                o_copy(step).wait_send()

            @pl.when(step < RING - 1)
            def _():
                for way in range(2):
                    for sub in range(subs):
                        rs_copy(step, way, sub).wait_send()
            return carry

        lax.fori_loop(0, RING, drain, 0)

    def normalise(values, gain):
        values = values.astype(jnp.float32)
        inv_rms = lax.rsqrt(jnp.mean(values * values, axis=-1, keepdims=True) + NORM_EPS)
        return (values * inv_rms * gain[...].astype(jnp.float32)).astype(jnp.bfloat16)

    def all_gather(buf, base_here, base_there, consume):
        def ag_copy(step, way, sub):
            slot = (step * 2 + way) * subs + sub
            here = buf.at[pl.ds(pl.multiple_of(base_here + piece_row(step, way), PIECE), PIECE), pl.ds(sub * cols, cols)]
            return remote(here, here, ag_send.at[slot], ag_recv.at[slot], ways[way][0])

        def fw_copy(step, way, sub):
            slot = (step * 2 + way) * subs + sub
            here = buf.at[pl.ds(pl.multiple_of(base_here + piece_row(step, way), PIECE), PIECE), pl.ds(sub * cols, cols)]
            there = buf.at[pl.ds(pl.multiple_of(base_there + piece_row(step, way), PIECE), PIECE), pl.ds(sub * cols, cols)]
            return remote(here, there, fw_send.at[slot], fw_recv.at[slot], peer)

        def two_steps(pair, carry):
            for odd in range(2):
                step = pair * 2 + odd
                for sub in range(subs):
                    for way in range(2):
                        if odd:
                            ag_copy(step - 1, way, sub).wait_recv()

                            @pl.when(pair < RING // 2 - 1)
                            def _():
                                ag_copy(step, way, sub).start()
                        else:
                            @pl.when(pair > 0)
                            def _():
                                ag_copy(step - 1, way, sub).wait_recv()

                            ag_copy(step, way, sub).start()
                        fw_copy(step, way, sub).start()
                    if consume is not None and sub % 2:
                        @pl.when(pair > 0)
                        def _():
                            do_part(pair - 1, odd * 2 + sub // 2)
            return carry

        def do_part(pair, part):
            if part == 0:
                for odd in range(2):
                    for way in range(2):
                        for sub in range(subs):
                            fw_copy(pair * 2 + odd, way, sub).wait_recv()
            consume(pair, part)

        lax.fori_loop(0, RING // 2, two_steps, 0)
        if consume is not None:
            for part in range(4):
                do_part(RING // 2 - 1, part)

        def drain(step, carry):
            for way in range(2):
                for sub in range(subs):
                    if consume is None:
                        fw_copy(step, way, sub).wait_recv()
                    fw_copy(step, way, sub).wait_send()

                    @pl.when(step < RING - 1)
                    def _():
                        ag_copy(step, way, sub).wait_send()
            return carry

        lax.fori_loop(0, RING, drain, 0)

    def finish_mid(rows, span, total):
        state[rows, span] = (hidden_ref[rows, span].astype(jnp.float32) + total).astype(jnp.bfloat16)

    reduce_scatter(True, wo, lambda i: wo_copy(i).wait(), finish_mid)
    b_full[pl.ds(pl.multiple_of(me * CHUNK, CHUNK), CHUNK), :] = normalise(state[...], gain_ref)
    down[pl.ds(ffn, down.shape[0] - ffn), :] = jnp.zeros((down.shape[0] - ffn, width), jnp.bfloat16)
    gate_copy.wait()
    up_copy.wait()
    down_copy.wait()

    def mlp_rows(pair, part):
        places = [(base, step, way) for base in (0, HALF) for step in range(2) for way in range(2)]
        dims = (((1,), (1,)), ((), ()))
        if part == 0:
            for i, (base, odd, way) in enumerate(places):
                at = pl.multiple_of(base + piece_row(pair * 2 + odd, way), PIECE)
                batch[pl.ds(i * PIECE, PIECE), :] = b_full[pl.ds(at, PIECE), :]
        elif part == 1:
            gate_pre[...] = lax.dot_general(gate[...], batch[...], dims, preferred_element_type=jnp.float32)
        elif part == 2:
            up_pre[...] = lax.dot_general(up[...], batch[...], dims, preferred_element_type=jnp.float32)
        else:
            hidden_act = jax.nn.silu(gate_pre[...]) * up_pre[...]
            padded = jnp.concatenate([hidden_act, jnp.zeros((act.shape[1] - ffn, 128), jnp.float32)], axis=0)
            turned = jnp.transpose(padded).astype(jnp.bfloat16)
            for i, (base, odd, way) in enumerate(places):
                at = pl.multiple_of(base + piece_row(pair * 2 + odd, way), PIECE)
                act[pl.ds(at, PIECE), :] = turned[i * PIECE:(i + 1) * PIECE]

    all_gather(b_full, 0, HALF, mlp_rows)

    def finish_out(rows, span, total):
        mixed = (state[rows, span].astype(jnp.float32) + total).astype(jnp.bfloat16)
        if last:
            own = pl.multiple_of(core * HALF + me * CHUNK + rows.start, PIECE)
            full_ref[pl.ds(own, PIECE), span] = mixed
        else:
            state_out[rows, span] = mixed

    reduce_scatter(False, down, None, finish_out)
    if last:
        all_gather(full_ref, core * HALF, core * HALF, None)
    else:
        normed_out[...] = normalise(state_out[...], next_ref)


def layer_call(call_id, layer, last, positions, q_lat, q_rope, c_new, k_new, w_uv, ckv_cache, kpe_cache, state, gain, next_gain, w_o, gate_t, up_t, w_down, scale):
    subs = 4
    seqs = 8
    width = state.shape[-1]
    ffn = gate_t.shape[1]
    padded = 384
    vmem = pl.BlockSpec(memory_space=pltpu.VMEM)
    hbm = pl.BlockSpec(memory_space=pl.ANY)
    small = [q_lat, q_rope, c_new, k_new, w_uv, state, gain] + ([] if last else [next_gain])
    shard = jax.ShapeDtypeStruct((CHUNK, width), jnp.bfloat16)
    outs = [jax.ShapeDtypeStruct((2 * HALF, width), jnp.bfloat16)] if last else [shard, shard]
    bf = lambda *shape: pltpu.VMEM(shape, jnp.bfloat16)
    dma = pltpu.SemaphoreType.DMA
    quarters = CHUNK // seqs
    mine = w_o.shape[1]
    scratch = ([] if last else [bf(2 * HALF, width)]) + [
        bf(quarters, seqs, *ckv_cache.shape[2:]), bf(quarters, seqs, *kpe_cache.shape[2:]), bf(RING, CHUNK, mine), bf(RING, CHUNK, mine), bf(RING, CHUNK, mine),
        bf(mine, width), bf(ffn, width), bf(ffn, width), bf(padded, width), bf(128, width), pltpu.VMEM((ffn, 128), jnp.float32), pltpu.VMEM((ffn, 128), jnp.float32), bf(2 * HALF, padded),
        bf(CHUNK, width), pltpu.VMEM((2, CHUNK, width), jnp.float32), bf(RING, CHUNK, width), bf(RING, CHUNK, width), bf(RING - 1, CHUNK, width), bf(RING - 1, CHUNK, width),
        dma((quarters,)), dma((quarters,)), dma((RING,)), dma((RING,)), dma((10,)), dma((RING,)), dma((RING,)),
        dma((14 * subs,)), dma((14 * subs,)), dma((14 * subs,)), dma((14 * subs,)), dma((16 * subs,)), dma((16 * subs,))]
    return pl.pallas_call(
        functools.partial(layer_kernel, layer, last, subs, scale),
        out_shape=outs,
        in_specs=[pl.BlockSpec(memory_space=pltpu.SMEM)] + [vmem] * len(small) + [hbm] * 6,
        out_specs=[vmem] * len(outs),
        scratch_shapes=scratch,
        compiler_params=pltpu.CompilerParams(collective_id=call_id, has_side_effects=True, vmem_limit_bytes=67043328),
        name='layer%d' % layer,
    )(positions, *small, ckv_cache, kpe_cache, w_o, gate_t, up_t, w_down)


def query_kernel(c_ref, cos_ref, sin_ref, own_q, peer_q, wk_ref, u_ref, r_ref):
    both_last = (((1,), (1,)), ((), ()))
    nope = wk_ref.shape[2]
    half = cos_ref.shape[1]
    for group, weight in enumerate((own_q, peer_q)):
        for h in range(weight.shape[1]):
            head = group * weight.shape[1] + h
            q = lax.dot_general(c_ref[...], weight[0, h], both_last, preferred_element_type=jnp.float32)
            lo, hi = q[:, nope:nope + half], q[:, nope + half:]
            r_ref[head] = jnp.concatenate([lo * cos_ref[...] - hi * sin_ref[...], hi * cos_ref[...] + lo * sin_ref[...]], axis=-1).astype(jnp.bfloat16)
            u_ref[head] = lax.dot_general(q[:, :nope].astype(jnp.bfloat16), wk_ref[head], both_last, preferred_element_type=jnp.float32).astype(jnp.bfloat16)


def query_call(layer, c_q, cos_part, sin_part, own_q, peer_q, w_k):
    rows = c_q.shape[0]
    heads, latent = w_k.shape[0], w_k.shape[1]
    rope = 2 * cos_part.shape[1]
    whole = lambda x: pl.BlockSpec(x.shape, lambda i: (0,) * x.ndim)
    picked = lambda x: pl.BlockSpec((1,) + x.shape[1:], lambda i: (layer, 0, 0, 0))
    outs = [jax.ShapeDtypeStruct((heads, rows, latent), jnp.bfloat16), jax.ShapeDtypeStruct((heads, rows, rope), jnp.bfloat16)]
    return pl.pallas_call(
        query_kernel,
        out_shape=outs,
        grid=(1,),
        in_specs=[whole(c_q), whole(cos_part), whole(sin_part), picked(own_q), picked(peer_q), whole(w_k)],
        out_specs=[whole(outs[0]), whole(outs[1])],
        compiler_params=pltpu.CompilerParams(vmem_limit_bytes=28 * 1024 * 1024),
        cost_estimate=pl.CostEstimate(flops=2 * rows * c_q.shape[1] * heads * 192, bytes_accessed=8 * 1024 * 1024, transcendentals=0),
        name='queries',
    )(c_q, cos_part, sin_part, own_q, peer_q, w_k)


def solution(mesh):
    cache_spec = P(None, 'dp', None, None)
    head_spec = P(None, None, 'tp', None)
    weight_specs = (P(), P(), P(), P(), P(), head_spec, head_spec, head_spec, P(None, 'tp', None, None), P(), P(None, None, 'tp'), P(None, None, 'tp'), P(None, 'tp', None))
    in_specs = (P('dp', None), P('dp'), cache_spec, cache_spec) + weight_specs
    out_specs = (P('dp', None), P(None, 'dp', None), P(None, 'dp', None))
    pairs = [(i, i + 1 - 2 * (i % 2)) for i in range(16)]

    def device_body(x_in, pos_ids, ckv_cache, kpe_cache, attn_gain, w_dq, q_gain, w_dkv, kv_gain, w_uq, w_uk, w_uv, w_o, mlp_gain, w_gate, w_up, w_down):
        core, me = ring_place()
        layers, latent = ckv_cache.shape[0], ckv_cache.shape[-1]
        width = x_in.shape[-1]
        nope = w_uk.shape[-1]
        lora = w_dq.shape[-1]
        scale = w_uq.shape[-1] ** -0.5
        first = core * HALF + me * CHUNK
        kpe_t = jnp.swapaxes(kpe_cache, 2, 3)
        gate_t = jnp.swapaxes(w_gate, 1, 2)
        up_t = jnp.swapaxes(w_up, 1, 2)
        w_o_flat = w_o.reshape(layers, -1, width)
        uq_t = jnp.transpose(w_uq, (0, 2, 3, 1))
        uk_t = jnp.transpose(w_uk, (0, 2, 1, 3))
        uv_t = jnp.transpose(w_uv, (0, 2, 1, 3))
        p_uq, p_uk, p_uv = [lax.ppermute(w, 'tp', pairs) for w in (uq_t, uk_t, uv_t)]
        state = lax.dynamic_slice_in_dim(x_in, first, CHUNK, 0)
        pos_rows = lax.dynamic_slice_in_dim(pos_ids, first, CHUNK, 0)
        pos_half = lax.dynamic_slice_in_dim(pos_ids, core * HALF, HALF, 0)
        half_rope = kpe_cache.shape[-1] // 2
        inv_freq = jnp.exp(jnp.arange(half_rope, dtype=jnp.float32) * (-math.log(ROPE_BASE) / half_rope))
        angles = pos_half.astype(jnp.float32)[:, None] * inv_freq
        cos_half, sin_half = jnp.cos(angles), jnp.sin(angles)
        c_rows = []
        k_rows = []
        for layer in range(layers):
            if layer == 0:
                normed = lax.optimization_barrier(rms_norm(lax.dynamic_slice_in_dim(x_in, core * HALF, HALF, 0), attn_gain[0]))
            own_pos = pos_half if layer == 0 else pos_rows
            c_q = rms_norm(jnp.dot(normed, w_dq[layer], preferred_element_type=jnp.float32), q_gain[layer])
            kv_lat = jnp.dot(normed, w_dkv[layer], preferred_element_type=jnp.float32)
            c_new = rms_norm(kv_lat[:, :latent], kv_gain[layer])
            k_new = rotary(kv_lat[:, latent:], own_pos).astype(jnp.bfloat16)
            if layer == 0:
                own_q, c_half, k_half = c_q, c_new, k_new
                rows = jnp.concatenate([c_new, k_new], axis=-1)
                peer_rows = lax.ppermute(rows, 'tp', pairs)
            else:
                pad = jnp.zeros((CHUNK, 64), jnp.bfloat16)
                shard = jnp.concatenate([c_q, c_new, k_new, pad], axis=-1)
                latents = gather_call(shard)
                own_q = latents[:HALF, :lora]
                c_half, k_half = latents[:HALF, lora:lora + latent], latents[:HALF, lora + latent:lora + latent + 64]
                rows, peer_rows = latents[:HALF, lora:lora + latent + 64], latents[HALF:, lora:lora + latent + 64]
            ordered = jnp.where(core == 0, jnp.concatenate([rows, peer_rows], axis=0), jnp.concatenate([peer_rows, rows], axis=0))
            c_rows.append(ordered[:, :latent])
            k_rows.append(ordered[:, latent:])
            w_k = jnp.concatenate([uk_t[layer], p_uk[layer]], axis=0)
            q_lat, q_rope = query_call(layer, own_q, cos_half, sin_half, uq_t, p_uq, w_k)
            q_lat, q_rope = jnp.transpose(q_lat, (1, 0, 2)), jnp.transpose(q_rope, (1, 0, 2))
            values = jnp.transpose(jnp.concatenate([uv_t[layer], p_uv[layer]], axis=0), (1, 0, 2)).reshape(latent, -1)
            last = layer + 1 == layers
            outs = layer_call(3 + layer, layer, last, pos_ids, q_lat, q_rope, c_half, k_half, values, ckv_cache, kpe_t, state, mlp_gain[layer][None],
                              None if last else attn_gain[layer + 1][None], w_o_flat, gate_t, up_t, w_down, scale)
            if last:
                x_out, = outs
            else:
                state, normed = outs
        return x_out, jnp.stack(c_rows), jnp.stack(k_rows)

    return jax.shard_map(device_body, mesh=mesh, in_specs=in_specs, out_specs=out_specs, check_vma=False)
```
